768 devices in a mesh: dp: 16 (over y, core), expert: 12 (over z), tensor: 4 (over x).
Axes of the slice: x: 4, y: 8, z: 12, core: 2. Of those that a mesh axis runs over, the one named last changes fastest.
Arguments:
- router_input: bfloat16 [24576, 2048], P(('dp', 'expert'), 'tensor'), may hold values from -6 to 6
- router_weight: bfloat16 [2048, 8], replicated, may hold values from -0.125 to 0.125
- expert_ids: int32 [24576, 2], P(('dp', 'expert', 'tensor')), may hold values from 0 to 7, all different within a row; in each aligned block of 32 rows (0 to 31, 32 to 63, ...) at most 9 rows name the same one
- down_weight: bfloat16 [61440, 2048], P(('expert', 'tensor')), may hold values from -0.0625 to 0.0625
- hidden: bfloat16 [16, 432, 61440], P('dp', None, ('expert', 'tensor')), may hold values from -6 to 6
- grad_output: bfloat16 [24576, 2048], P(('dp', 'expert', 'tensor')), may hold values from -4 to 4
Outputs:
- weight_grad: bfloat16 [61440, 2048], P(('expert', 'tensor', 'dp'))
- hidden_grad: bfloat16 [16, 432, 61440], P('dp', None, ('expert', 'tensor'))
- router_grad: float32 [2048, 8], replicated
- input_grad: bfloat16 [24576, 2048], P(('dp', 'expert', 'tensor'))
The draws below stay inside these ranges and needn't reach their ends.
Inputs may be any that keep to these rules, and one draw needn't show every extreme that they name: `expert_ids`: each row names 2 different experts. Within the 32 rows of one device no expert is named more than 9 times, and some device's rows name some expert exactly 9 times.
All inputs are finite; a program needn't handle non-finite values.
Results may differ from the reference program's by a relative error of at most 0.018.
Values may be sent and summed in bfloat16 or wider, within the bound.
A program may use at most 64 MiB of HBM per device.

```python
import math
import jax
import jax.numpy as jnp
import numpy as np
from jax import lax

D = 2048
FF = 7680
EXPERTS = 8
TOPK = 2
TOK_DEV = 32
CAP = 9
SOURCES = 48
TOKENS = 24576
N_DP = 16


def shard_levels(key, shape, split, smallest, largest):
    level, own = 1.0, jax.random.fold_in(key, 6)
    for axis_at, blocks in split:
        draws = jnp.exp(jax.random.uniform(jax.random.fold_in(own, axis_at), (blocks,), jnp.float32, smallest / len(split), largest / len(split)))
        level = level * jnp.repeat(draws, shape[axis_at] // blocks).reshape([-1 if axis == axis_at else 1 for axis in range(len(shape))])
    return level


def deal_out(key, own, number, rows, amount, top, most, slope):
    order = jax.random.permutation(key, amount)
    crowded, common = shares(amount, rows * top, most, slope, True), shares(amount, rows * top, most, slope, False)
    places = jnp.arange(amount)

    def named(tallies, offset_by):
        used = int((tallies > 0).sum())
        fixed = max(1, used // 4)
        shifted = fixed + (places - fixed + offset_by * (used - fixed)) % max(1, amount - fixed)
        return jnp.zeros((amount,), jnp.int32).at[order[jnp.where(places < fixed, places, shifted)]].set(jnp.asarray(tallies, jnp.int32))

    tallies = jnp.where(number % 4 == 0, named(crowded, number // 4), named(common, number - number // 4 - 1))
    mixed = jax.random.permutation(jax.random.fold_in(own, 3), amount)
    donor, receiver = mixed[0:amount // 2 * 2:2], mixed[1:amount // 2 * 2:2]
    slack = jnp.minimum(tallies[donor] - 1, most - tallies[receiver]) // 2
    slack = jnp.where((donor == order[0]) | (receiver == order[0]) | (tallies[receiver] == 0), 0, jnp.maximum(slack, 0))
    shifted = jax.random.randint(jax.random.fold_in(own, 4), (amount // 2,), 0, 1 << 20) % (slack + 1)
    tallies = tallies.at[donor].add(-shifted).at[receiver].add(shifted)
    items = jnp.searchsorted(jnp.cumsum(tallies), jnp.arange(rows * top), side="right").astype(jnp.int32)
    listing = items.reshape(top, rows).T
    listing = listing[jax.random.permutation(jax.random.fold_in(own, 1), rows)]
    offset_by = jax.random.randint(jax.random.fold_in(own, 2), (rows, 1), 0, top)
    return jnp.take_along_axis(listing, (jnp.arange(top)[None, :] + offset_by) % top, axis=1)


def shares(count, total, bound, slope, full):
    weights = [(1 << 20) // math.isqrt(grade ** slope) + 1 for grade in range(1, count + 1)]
    largest = bound if full else min(bound, max(-(-total // count), total * weights[0] // sum(weights)))
    least = 1 if total - largest >= count - 1 else 0
    given, spare = [largest] + [least] * (count - 1), total - largest - least * (count - 1)
    while spare > 0:
        movable = [i for i in range(1, count) if given[i] < largest] or [i for i in range(1, count) if given[i] < bound]
        mass, left = sum([weights[i] for i in movable]), spare
        for i in movable:
            extra = min(bound - given[i], max(1, left * weights[i] // mass), spare)
            given[i] = given[i] + extra
            spare = spare - extra
    return np.array(given)


def centred(stream_key, dims, spread, bound, cuts=(), kind=jnp.bfloat16):
    drawn = jax.random.normal(stream_key, dims, jnp.float32) * spread
    if len(cuts) > 0:
        drawn = shard_levels(stream_key, dims, cuts, -0.22, 0.18) * drawn
    return jnp.clip(drawn, min=-bound, max=bound).astype(kind)


def setup_inputs(seed: int = 0) -> dict:
    splits = jax.random.split(jax.random.key(seed), 7)
    router_input = centred(splits[0], (TOKENS, D), 1.0, 6.0, ((0, 192), (1, 4)))
    router_weight = centred(splits[1], (D, EXPERTS), D ** -0.5, 0.125)
    expert_ids_keys = jax.random.split(jax.random.fold_in(splits[2], 1), TOKENS // TOK_DEV)
    expert_ids_turns = jax.random.permutation(jax.random.fold_in(splits[2], 3), TOKENS // TOK_DEV)
    expert_ids = jax.vmap(lambda own, number: deal_out(jax.random.fold_in(splits[2], 2), own, number, TOK_DEV, EXPERTS, TOPK, CAP, 2))(expert_ids_keys, expert_ids_turns).reshape((TOKENS, TOPK))
    down_weight = centred(splits[3], (EXPERTS * FF, D), FF ** -0.5, 0.0625, ((0, 48),))
    hidden = centred(splits[4], (N_DP, SOURCES * CAP, EXPERTS * FF), 1.0, 6.0, ((0, 16), (2, 48)))
    grad_output = centred(splits[5], (TOKENS, D), 0.25, 4.0, ((0, 768),))
    return dict(router_input=router_input, router_weight=router_weight, expert_ids=expert_ids, down_weight=down_weight, hidden=hidden, grad_output=grad_output)


def reference(router_input, router_weight, expert_ids, down_weight, hidden, grad_output):
    logits = jnp.dot(router_input, router_weight, preferred_element_type=jnp.float32)
    labels = jnp.arange(EXPERTS, dtype=jnp.int32)
    onehot_int = (expert_ids[:, :, None] == labels).astype(jnp.int32)
    onehot = onehot_int.astype(jnp.float32)
    picked = jnp.sum(onehot * logits[:, None, :], axis=2)
    first_gate = jax.nn.sigmoid(picked[:, 0] - picked[:, 1])
    second_gate = jax.nn.sigmoid(picked[:, 1] - picked[:, 0])
    gate_values = jnp.stack([first_gate, second_gate], axis=1)
    gate_low = gate_values.astype(jnp.bfloat16)
    blocks = TOKENS // TOK_DEV
    flat_hits = onehot_int.reshape(blocks, TOK_DEV * TOPK, EXPERTS)
    before = jnp.cumsum(flat_hits, axis=1) - flat_hits
    slot_pos = jnp.sum(before * flat_hits, axis=2).reshape(blocks, TOK_DEV, TOPK)
    slot_ids = jnp.arange(CAP, dtype=jnp.int32)
    dispatch_table = onehot.reshape(blocks, TOK_DEV, TOPK, EXPERTS, 1) * (slot_pos[:, :, :, None, None] == slot_ids).astype(jnp.float32)
    table_groups = dispatch_table.reshape(N_DP, SOURCES, TOK_DEV, TOPK, EXPERTS, CAP)
    grad_groups = grad_output.reshape(N_DP, SOURCES, TOK_DEV, D)
    gate_groups = gate_low.reshape(N_DP, SOURCES, TOK_DEV, TOPK)
    expert_weights = down_weight.reshape(EXPERTS, FF, D)

    def one_expert(pieces):
        expert_grad, expert_gate, expert_hidden, expert_weight = pieces
        expert_image = jnp.dot(expert_grad, expert_weight.T, preferred_element_type=jnp.float32)
        hidden_part = (expert_gate[:, None] * expert_image).astype(jnp.bfloat16)
        gate_part = jnp.sum(expert_hidden.astype(jnp.float32) * expert_image, axis=1)
        gated = (expert_gate[:, None] * expert_grad.astype(jnp.float32)).astype(jnp.bfloat16)
        weight_term = jnp.dot(expert_hidden.T, gated, preferred_element_type=jnp.float32).astype(jnp.bfloat16)
        return hidden_part, gate_part, weight_term

    def one_group(running_total, pieces):
        table_i, grad_i, gate_i, hidden_i = pieces
        slot_table = jnp.sum(table_i, axis=2)
        packed_grad = jnp.einsum("srec,srd->escd", slot_table, grad_i.astype(jnp.float32))
        packed_grad = packed_grad.astype(jnp.bfloat16).reshape(EXPERTS, SOURCES * CAP, D)
        packed_gate = jnp.einsum("srkec,srk->esc", table_i, gate_i.astype(jnp.float32)).reshape(EXPERTS, SOURCES * CAP)
        hidden_split = hidden_i.reshape(SOURCES * CAP, EXPERTS, FF).transpose(1, 0, 2)
        hidden_part, gate_part, weight_term = lax.map(one_expert, (packed_grad, packed_gate, hidden_split, expert_weights))
        running_total = running_total + weight_term.reshape(EXPERTS * FF, D).astype(jnp.float32)
        token_grad = jnp.einsum("srkec,esc->srk", table_i, gate_part.reshape(EXPERTS, SOURCES, CAP))
        hidden_rows = hidden_part.transpose(1, 0, 2).reshape(SOURCES * CAP, EXPERTS * FF)
        return running_total, (hidden_rows, token_grad)

    zero_total = jnp.zeros((EXPERTS * FF, D), jnp.float32)
    running_total, outputs = lax.scan(one_group, zero_total, (table_groups, grad_groups, gate_groups, hidden))
    hidden_grad, token_grad = outputs
    weight_grad = running_total.astype(jnp.bfloat16)
    gate_grad = token_grad.reshape(TOKENS, TOPK)
    mixed_term = jnp.sum(gate_values * gate_grad, axis=1, keepdims=True)
    logit_part = gate_values * (gate_grad - mixed_term)
    logit_grad = jnp.sum(onehot * logit_part[:, :, None], axis=1)
    input_grad = jnp.dot(logit_grad, router_weight.astype(jnp.float32).T, precision=lax.Precision.HIGHEST).astype(jnp.bfloat16)
    router_grad = jnp.dot(router_input.astype(jnp.float32).T, logit_grad, precision=lax.Precision.HIGHEST)
    return weight_grad, hidden_grad, router_grad, input_grad
```

```python
import functools

import jax
import jax.numpy as jnp
from jax import lax
from jax.experimental import pallas as pl
from jax.experimental.pallas import tpu as pltpu
from jax.sharding import Mesh
from jax.sharding import PartitionSpec as P

F32 = jnp.float32
BF16 = jnp.bfloat16
I32 = jnp.int32
HIGH = lax.Precision.HIGHEST
NT = (((1,), (1,)), ((), ()))

DP = ("dp_0", "dp_1")
DP_EXPERT_TENSOR = ("dp_0", "dp_1", "expert", "tensor")
DP_EXPERT = ("dp_0", "dp_1", "expert")
EXPERT_TENSOR_DP = ("expert", "tensor", "dp_0", "dp_1")

NY, NC, NZ, NX = 8, 2, 12, 4
NE = 8
CAP = 9
TOK = 32
NQ = 4
LB = 4
QC = LB * 128
RP = 40
RX = 112
ROWS = NX * RX
ZORDER = (6, 7, 5, 8, 4, 9, 3, 10, 2, 11, 1)
PLUS, MINUS = 0, 1
RS_SLOT = {}
for _s in range(4):
    for _dir, _half, _n in ((PLUS, 0, 4), (MINUS, 1, 4), (PLUS, 1, 3), (MINUS, 0, 3)):
        if _s < _n:
            RS_SLOT[(_dir, _half, _s)] = len(RS_SLOT)
NRS = len(RS_SLOT)


def iota(shape, dim):
    return lax.broadcasted_iota(I32, shape, dim)


def onehot(mask):
    return jnp.where(mask, 1.0, 0.0).astype(BF16)


def dot(a, b, dims=(((1,), (0,)), ((), ())), precision=None):
    return lax.dot_general(a, b, dims, precision=precision, preferred_element_type=F32)


def kernel(
    ids_ref, rin_ref, rwt_ref, grad_ref, down_hbm, hid_hbm,
    wg_ref, hg_hbm, rg_ref, ig_ref,
    down, hid, hidp, hidt, image, hg, gcol, relay_r,
    chunk, zbuf, xsend, xbuf,
    logit_buf, pg_send, pg_buf, pgx_send, pgx_buf,
    gx_send, gx_buf, gz_send, gz_buf, lg_buf,
    rp_send, rc_buf, ry_send, ry_buf, rz_send, rz_buf, rx_send, rx_buf,
    wbuf, dbuf, rsbuf,
    load_sem, out_sem,
    zs_sem, zr_sem, xs_sem, xr_sem,
    small_s, small_r,
    d_s, d_r, rs_s, rs_r,
):
    y, c = lax.axis_index("dp_0"), lax.axis_index("dp_1")
    z, x = lax.axis_index("expert"), lax.axis_index("tensor")
    oc = 1 - c
    e_lo, e_hi = (z * NX) // 6, (z * NX + NX - 1) // 6
    middle = lax.rem(z, 3) == 1
    sel_hi = lax.rem(z, 3) * (2 - lax.rem(z, 3))
    zpeers = [lax.rem(z + k, NZ) for k in ZORDER]
    xpeers = [lax.rem(x + k, NX) for k in (2, 1, 3)]
    ypeers = [lax.rem(y + k, NY) for k in (4, 5, 3, 6, 2, 7, 1)]
    up, dn = lax.rem(y + 1, NY), lax.rem(y + NY - 1, NY)

    def load(src, dst, i):
        return pltpu.make_async_copy(src, dst, load_sem.at[i])

    load(hid_hbm, hid, 0).start()
    load(down_hbm, down, 1).start()

    def send(src, dst, s_sem, r_sem, **where):
        pltpu.make_async_remote_copy(
            src_ref=src, dst_ref=dst, send_sem=s_sem, recv_sem=r_sem,
            device_id=where, device_id_type=pl.DeviceIdType.MESH,
        ).start()

    def wait(ref, sem):
        pltpu.make_async_copy(ref, ref, sem).wait()

    barrier = pltpu.get_barrier_semaphore()

    def greet(**where):
        pl.semaphore_signal(barrier, inc=1, device_id=where, device_id_type=pl.DeviceIdType.MESH)

    for p in zpeers:
        greet(expert=p)
    for p in xpeers:
        greet(tensor=p)
        greet(tensor=p, dp_1=oc)
    for p in ypeers:
        greet(dp_0=p)
    greet(dp_1=oc)

    sub8, lane8 = iota((8, 128), 0), iota((8, 128), 1)
    ids = [ids_ref[0:1, :], ids_ref[1:2, :]]
    hit = [sub8 == ids[k] for k in range(2)]
    hits = (jnp.where(hit[0], 1.0, 0.0) + jnp.where(hit[1], 1.0, 0.0)).astype(BF16)
    r128, l128 = iota((128, 128), 0), iota((128, 128), 1)
    tri = onehot((r128 < l128) & (r128 // TOK == l128 // TOK))
    before = dot(hits, tri)
    pos = [jnp.sum(jnp.where(hit[k], before, 0.0), axis=0, keepdims=True).astype(I32) for k in range(2)]
    lane1 = iota((1, 128), 1)
    target = [ids[k] * RP + (lane1 // TOK) * CAP + pos[k] for k in range(2)]
    slot_at = [r128 == pos[k] for k in range(2)]
    part = dot(rwt_ref[:, pl.ds(pl.multiple_of(x * 512, 512), 512)], rin_ref[...], NT)
    logit_buf[x] = part
    pack_rows = iota((NE * RP, 128), 0)
    table = onehot((pack_rows == target[0]) | (pack_rows == target[1]))
    for q in range(NQ):
        stack = jnp.concatenate(
            [grad_ref[:, q * QC + b * 128 : q * QC + (b + 1) * 128] for b in range(LB)], axis=0
        )
        packed = dot(table, stack).astype(BF16)
        for e in range(NE):
            chunk[q, e] = packed[e * RP : (e + 1) * RP]

    pl.semaphore_wait(barrier, len(zpeers) + 2 * len(xpeers) + len(ypeers) + 1)

    for p in xpeers:
        send(logit_buf.at[x], logit_buf.at[x], small_s.at[0], small_r.at[0], tensor=p)

    def z_send(q):
        for p in zpeers:
            lo, hi = (p * NX) // 6, (p * NX + NX - 1) // 6
            send(chunk.at[q, lo], zbuf.at[0, q, z], zs_sem.at[0, q], zr_sem.at[0, q], expert=p)

            @pl.when(lax.rem(p, 3) == 1)
            def _():
                send(chunk.at[q, hi], zbuf.at[1, q, z], zs_sem.at[1, q], zr_sem.at[1, q], expert=p)

    z_send(0)
    for q in range(NQ):
        zbuf[0, q, z] = chunk[q, e_lo]
        zbuf[1, q, z] = chunk[q, e_hi]

    others = lambda ref, n: ref.at[0 : n - 1]
    wait(others(logit_buf, NX), small_r.at[0])
    logits = logit_buf[0] + logit_buf[1] + logit_buf[2] + logit_buf[3]
    picked = [jnp.sum(jnp.where(hit[k], logits, 0.0), axis=0, keepdims=True) for k in range(2)]
    own_lanes = lane1 // TOK == x

    def spread(row):
        row = jnp.broadcast_to(jnp.where(own_lanes, row, 0.0), (8, 128))
        row = row + pltpu.roll(row, TOK, 1)
        return row + pltpu.roll(row, 2 * TOK, 1)

    gate = [
        spread(jax.nn.sigmoid(picked[0] - picked[1])),
        spread(jax.nn.sigmoid(picked[1] - picked[0])),
    ]
    first = lane8 < TOK
    packed_gate = dot(
        jnp.where(hit[0] & first, gate[0], 0.0).astype(BF16), onehot(slot_at[0]), NT
    ) + dot(jnp.where(hit[1] & first, gate[1], 0.0).astype(BF16), onehot(slot_at[1]), NT)
    pg_send[...] = packed_gate
    pg_buf[z] = packed_gate
    for p in zpeers:
        send(pg_send, pg_buf.at[z], small_s.at[1], small_r.at[1], expert=p)
    z_send(1)
    z_send(2)
    z_send(3)

    rr, kk = iota((RX, NZ * RP), 0), iota((RX, NZ * RP), 1)
    for b in range(LB):
        relay_r[b] = onehot((kk == (rr // CAP) * RP + b * CAP + lax.rem(rr, CAP)) & (rr < NZ * CAP))

    def z_relay(q):
        wait(others(zbuf.at[0, q], NZ), zr_sem.at[0, q])

        @pl.when(middle)
        def _():
            wait(others(zbuf.at[1, q], NZ), zr_sem.at[1, q])

        for cls in range(2):
            rows = zbuf[0 if cls == 0 else sel_hi, q].reshape(NZ * RP, 128)
            for b in range(LB):
                xsend[cls, q, :, b * 128 : (b + 1) * 128] = dot(relay_r[b], rows).astype(BF16)
        for p in xpeers:
            send(xsend.at[p // 2, q], xbuf.at[q, x], xs_sem.at[q], xr_sem.at[q], tensor=p)
        xbuf[q, x] = xsend[x // 2, q]

    load(hid_hbm, hid, 0).wait()
    r1, m1 = iota((ROWS, NX * NZ * CAP), 0), iota((ROWS, NX * NZ * CAP), 1)
    in_col = lax.rem(r1, RX)
    perm = onehot(
        (m1 == ((in_col // CAP) * NX + r1 // RX) * CAP + lax.rem(in_col, CAP)) & (in_col < NZ * CAP)
    )
    hidp[...] = dot(perm, hid[...]).astype(BF16)
    hidt[...] = hidp[...].T

    z_relay(0)

    wait(others(pg_buf, NZ), small_r.at[1])
    sub3 = iota((NZ, 8, 128), 1)
    for cls, e in ((0, e_lo), (1, e_hi)):
        pgx_send[cls] = jnp.zeros((16, 128), F32)
        pgx_send[cls, 0:NZ] = jnp.sum(jnp.where(sub3 == e, pg_buf[...], 0.0), axis=1)
    for p in xpeers:
        send(pgx_send.at[p // 2], pgx_buf.at[x], small_s.at[2], small_r.at[2], tensor=p)
    pgx_buf[x] = pgx_send[x // 2]

    z_relay(1)

    rq, lq = iota((ROWS, 64), 0), iota((ROWS, 64), 1)
    qc = lax.rem(rq, RX)
    column_of = onehot((lq == (rq // RX) * 16 + qc // CAP) & (qc < NZ * CAP))
    rw, lw = iota((ROWS, 128), 0), iota((ROWS, 128), 1)
    own_slot = lw == lax.rem(lax.rem(rw, RX), CAP)

    def make_gates():
        wait(others(pgx_buf, NX), small_r.at[2])
        spread_gate = dot(column_of, pgx_buf[...].reshape(64, 128).astype(BF16))
        column = jnp.sum(jnp.where(own_slot, spread_gate, 0.0), axis=1, keepdims=True)
        gcol[...] = jnp.broadcast_to(column, (ROWS, 128))

    def x_wait(q):
        wait(others(xbuf.at[q], NX), xr_sem.at[q])

    def image_part(q):
        part = dot(xbuf[q].reshape(ROWS, QC), down[:, q * QC : (q + 1) * QC], NT)
        if q == 0:
            image[...] = part
        else:
            image[...] += part

    def weight_part(q):
        rows = xbuf[q].reshape(ROWS, QC).astype(F32)
        gated = (gcol[:, 0:1] * rows).astype(BF16)
        term = dot(hidt[...], gated).astype(BF16)
        for yy in range(NY):
            for cc in range(NC):
                at = (yy * NC + cc) * 80
                wbuf[q, cc, yy] = term[at : at + 80]
        send(wbuf.at[q, oc], dbuf.at[q], d_s.at[q], d_r.at[q], dp_1=oc)

    def cols(half):
        return pl.ds(half * (QC // 2), QC // 2)

    def y_send(q, src, d, half, s):
        slot = RS_SLOT[(d, half, s)]
        send(src, rsbuf.at[q, slot], rs_s.at[q], rs_r.at[q, slot], dp_0=up if d == PLUS else dn)

    def rs_first(q):
        wait(dbuf.at[q], d_r.at[q])
        dbuf[q] = (wbuf[q, c].astype(F32) + dbuf[q].astype(F32)).astype(BF16)
        for d, half, far in ((PLUS, 0, 4), (MINUS, 1, 4), (PLUS, 1, 3), (MINUS, 0, 5)):
            y_send(q, dbuf.at[q, lax.rem(y + far, NY), :, cols(half)], d, half, 0)

    def rs_step(q, s):
        for d, half, n, off in (
            (PLUS, 0, 4, 3 - s), (MINUS, 1, 4, 5 + s), (PLUS, 1, 3, 2 - s), (MINUS, 0, 3, 6 + s),
        ):
            if s >= n:
                continue
            slot = RS_SLOT[(d, half, s)]
            wait(rsbuf.at[q, slot], rs_r.at[q, slot])
            if s == n - 1:
                continue
            block = dbuf[q, lax.rem(y + off, NY), :, half * (QC // 2) : (half + 1) * (QC // 2)]
            rsbuf[q, slot] = (rsbuf[q, slot].astype(F32) + block.astype(F32)).astype(BF16)
            y_send(q, rsbuf.at[q, slot], d, half, s + 1)
        if s == 3:
            for half in range(2):
                lo = half * (QC // 2)
                a = rsbuf[q, RS_SLOT[(PLUS, half, 3 - half)]].astype(F32)
                b = rsbuf[q, RS_SLOT[(MINUS, half, 2 + half)]].astype(F32)
                mine = dbuf[q, y, :, lo : lo + QC // 2].astype(F32)
                wg_ref[:, q * QC + lo : q * QC + lo + QC // 2] = (mine + a + b).astype(BF16)

    make_gates()
    x_wait(0)
    weight_part(0)
    load(down_hbm, down, 1).wait()
    image_part(0)
    z_relay(2)
    rs_first(0)
    x_wait(1)
    weight_part(1)
    image_part(1)
    z_relay(3)
    rs_step(0, 0)
    rs_first(1)
    x_wait(2)
    image_part(2)
    weight_part(2)
    rs_step(0, 1)
    rs_step(1, 0)
    x_wait(3)
    image_part(3)

    slot_sum = jnp.sum(hidp[...].astype(F32) * image[...], axis=1, keepdims=True)
    rt, lt = iota((64, ROWS), 0), iota((64, ROWS), 1)
    tc = lax.rem(lt, RX)
    back = jnp.where((rt == (lt // RX) * 16 + tc // CAP) & (tc < NZ * CAP), 1.0, 0.0)
    slots = dot(back, jnp.where(own_slot, slot_sum, 0.0), precision=HIGH)
    for p in range(NX):
        gx_send[p] = slots[p * 16 : (p + 1) * 16]
    gx_buf[x] = gx_send[x]
    for p in xpeers:
        send(gx_send.at[p], gx_buf.at[x], small_s.at[3], small_r.at[3], tensor=p)

    weight_part(3)
    rs_first(2)

    wait(others(gx_buf, NX), small_r.at[3])
    sum_lo, sum_hi = gx_buf[0] + gx_buf[1], gx_buf[2] + gx_buf[3]
    for p in range(NZ):
        gz_send[p] = jnp.where(sub8 == e_lo, sum_lo[p : p + 1], 0.0) + jnp.where(
            sub8 == e_hi, sum_hi[p : p + 1], 0.0
        )
    gz_buf[z] = gz_send[z]
    for p in zpeers:
        send(gz_send.at[p], gz_buf.at[z], small_s.at[4], small_r.at[4], expert=p)

    rs_step(0, 2)
    rs_step(1, 1)
    rs_first(3)

    scaled = (gcol[:, 0:1] * image[...]).astype(BF16)
    m2, r2 = iota((NX * NZ * CAP, ROWS), 0), iota((NX * NZ * CAP, ROWS), 1)
    unperm = onehot(r2 == lax.rem(m2 // CAP, NX) * RX + (m2 // (CAP * NX)) * CAP + lax.rem(m2, CAP))
    hg[...] = dot(unperm, scaled).astype(BF16)
    out_copy = pltpu.make_async_copy(hg, hg_hbm, out_sem)
    out_copy.start()

    rs_step(2, 0)

    wait(others(gz_buf, NZ), small_r.at[4])
    sums = gz_buf[0]
    for p in range(1, NZ):
        sums = sums + gz_buf[p]
    gate_grad = []
    for k in range(2):
        at_slot = dot(sums, jnp.where(slot_at[k], 1.0, 0.0), precision=HIGH)
        gate_grad.append(jnp.sum(jnp.where(hit[k], at_slot, 0.0), axis=0, keepdims=True))
    mixed = gate[0] * gate_grad[0] + gate[1] * gate_grad[1]
    logit_grad = jnp.where(hit[0], gate[0] * (gate_grad[0] - mixed), 0.0) + jnp.where(
        hit[1], gate[1] * (gate_grad[1] - mixed), 0.0
    )
    lg_buf[x] = jnp.where(lane8 // TOK == x, logit_grad, 0.0)
    for p in xpeers:
        send(lg_buf.at[x], lg_buf.at[x], small_s.at[5], small_r.at[5], tensor=p)
    tall = jnp.where(r128 // 8 == 0, jnp.concatenate([logit_grad] * 16, axis=0), 0.0).T
    ig_ref[...] = dot(tall[0:TOK, 0:8], rwt_ref[...].astype(F32), precision=HIGH).astype(BF16)

    rs_step(0, 3)
    rs_step(1, 2)

    wait(others(lg_buf, NX), small_r.at[5])
    group_grad = lg_buf[0] + lg_buf[1] + lg_buf[2] + lg_buf[3]
    router = dot(group_grad, rin_ref[...].astype(F32), precision=HIGH)
    rp_send[0] = router[:, 0:256]
    rp_send[1] = router[:, 256:512]
    send(rp_send.at[oc], rc_buf, small_s.at[6], small_r.at[6], dp_1=oc)

    rs_step(2, 1)
    rs_step(3, 0)

    wait(rc_buf, small_r.at[6])
    pair = rp_send[c] + rc_buf[...]
    ry_send[...] = pair
    ry_buf[y] = pair
    for p in ypeers:
        send(ry_send, ry_buf.at[y], small_s.at[7], small_r.at[7], dp_0=p)
    rs_step(1, 3)
    rs_step(2, 2)
    wait(others(ry_buf, NY), small_r.at[7])
    total = ry_buf[0]
    for p in range(1, NY):
        total = total + ry_buf[p]
    rz_send[...] = total
    rz_buf[z] = total
    for p in zpeers:
        send(rz_send, rz_buf.at[z], small_s.at[8], small_r.at[8], expert=p)
    rs_step(3, 1)
    rs_step(2, 3)
    wait(others(rz_buf, NZ), small_r.at[8])
    total = rz_buf[0]
    for p in range(1, NZ):
        total = total + rz_buf[p]
    rx_send[...] = total
    here = x * NC + c
    rx_buf[here] = total
    for p in xpeers:
        for cc in (c, oc):
            send(rx_send, rx_buf.at[here], small_s.at[9], small_r.at[9], tensor=p, dp_1=cc)
    send(rx_send, rx_buf.at[here], small_s.at[9], small_r.at[9], dp_1=oc)
    rs_step(3, 2)
    rs_step(3, 3)
    wait(others(rx_buf, NX * NC), small_r.at[9])
    rg_ref[...] = rx_buf[...]

    for q in range(NQ):
        wait(others(zbuf.at[0, q], NZ), zs_sem.at[0, q])

        @pl.when(middle)
        def _():
            wait(zbuf.at[1, q, 0:3], zs_sem.at[1, q])

        @pl.when(jnp.logical_not(middle))
        def _():
            wait(zbuf.at[1, q, 0:4], zs_sem.at[1, q])

        wait(others(xbuf.at[q], NX), xs_sem.at[q])
        wait(dbuf.at[q], d_s.at[q])
        wait(rsbuf.at[q], rs_s.at[q])
    wait(others(logit_buf, NX), small_s.at[0])
    wait(others(pg_buf, NZ), small_s.at[1])
    wait(others(pgx_buf, NX), small_s.at[2])
    wait(others(gx_buf, NX), small_s.at[3])
    wait(others(gz_buf, NZ), small_s.at[4])
    wait(others(lg_buf, NX), small_s.at[5])
    wait(rc_buf, small_s.at[6])
    wait(others(ry_buf, NY), small_s.at[7])
    wait(others(rz_buf, NZ), small_s.at[8])
    wait(others(rx_buf, NX * NC), small_s.at[9])
    out_copy.wait()


def per_device(router_input, router_weight, expert_ids, down_weight, hidden, grad_output):
    ids = jnp.pad(jnp.tile(expert_ids.T, (1, 128 // TOK)), ((0, 6), (0, 0)))
    rwt = router_weight.T
    slots, units = hidden.shape[1], hidden.shape[2]
    width = grad_output.shape[1]
    vmem = pl.BlockSpec(memory_space=pltpu.VMEM)
    hbm = pl.BlockSpec(memory_space=pl.ANY)
    V = pltpu.VMEM
    dma = pltpu.SemaphoreType.DMA
    weight_grad, hidden_grad, router, input_grad = pl.pallas_call(
        kernel,
        out_shape=(
            jax.ShapeDtypeStruct((units // (NY * NC), width), BF16),
            jax.ShapeDtypeStruct((slots, units), BF16),
            jax.ShapeDtypeStruct((NX * NC, 8, 256), F32),
            jax.ShapeDtypeStruct((TOK, width), BF16),
        ),
        in_specs=[vmem, vmem, vmem, vmem, hbm, hbm],
        out_specs=(vmem, hbm, vmem, vmem),
        scratch_shapes=[
            V((units, width), BF16),
            V((slots, units), BF16),
            V((ROWS, units), BF16),
            V((units, ROWS), BF16),
            V((ROWS, units), F32),
            V((slots, units), BF16),
            V((ROWS, 128), F32),
            V((LB, RX, NZ * RP), BF16),
            V((NQ, NE, RP, 128), BF16),
            V((2, NQ, NZ, RP, 128), BF16),
            V((2, NQ, RX, QC), BF16),
            V((NQ, NX, RX, QC), BF16),
            V((NX, 8, 128), F32),
            V((8, 128), F32),
            V((NZ, 8, 128), F32),
            V((2, 16, 128), F32),
            V((NX, 16, 128), F32),
            V((NX, 16, 128), F32),
            V((NX, 16, 128), F32),
            V((NZ, 8, 128), F32),
            V((NZ, 8, 128), F32),
            V((NX, 8, 128), F32),
            V((2, 8, 256), F32),
            V((8, 256), F32),
            V((8, 256), F32),
            V((NY, 8, 256), F32),
            V((8, 256), F32),
            V((NZ, 8, 256), F32),
            V((8, 256), F32),
            V((NX * NC, 8, 256), F32),
            V((NQ, NC, NY, 80, QC), BF16),
            V((NQ, NY, 80, QC), BF16),
            V((NQ, NRS, 80, QC // 2), BF16),
            dma((2,)), dma,
            dma((2, NQ)), dma((2, NQ)), dma((NQ,)), dma((NQ,)),
            dma((10,)), dma((10,)),
            dma((NQ,)), dma((NQ,)), dma((NQ,)), dma((NQ, NRS)),
        ],
        compiler_params=pltpu.CompilerParams(
            collective_id=0, has_side_effects=True, vmem_limit_bytes=60 * 1024 * 1024
        ),
    )(ids, router_input, rwt, grad_output, down_weight, hidden[0])
    router_grad = jnp.transpose(router, (0, 2, 1)).reshape(width, 8)
    return weight_grad, hidden_grad[None], router_grad, input_grad


def solution(mesh):
    finer = Mesh(
        mesh.devices.reshape(NY, NC, mesh.shape["expert"], mesh.shape["tensor"]),
        ("dp_0", "dp_1", "expert", "tensor"),
    )
    placed = (
        P(DP_EXPERT, "tensor"),
        P(),
        P(DP_EXPERT_TENSOR, None),
        P(("expert", "tensor"), None),
        P(DP, None, ("expert", "tensor")),
        P(DP_EXPERT_TENSOR, None),
    )
    return jax.shard_map(
        per_device,
        mesh=finer,
        in_specs=placed,
        out_specs=(
            P(EXPERT_TENSOR_DP, None),
            P(DP, None, ("expert", "tensor")),
            P(),
            P(DP_EXPERT_TENSOR, None),
        ),
        check_vma=False,
    )
```

```python
import functools

import jax
import jax.numpy as jnp
from jax import lax
from jax.experimental import pallas as pl
from jax.experimental.pallas import tpu as pltpu
from jax.sharding import Mesh
from jax.sharding import PartitionSpec as P

F32 = jnp.float32
BF16 = jnp.bfloat16
I32 = jnp.int32
HIGH = lax.Precision.HIGHEST
NT = (((1,), (1,)), ((), ()))

DP = ("dp_0", "dp_1")
DP_EXPERT_TENSOR = ("dp_0", "dp_1", "expert", "tensor")
DP_EXPERT = ("dp_0", "dp_1", "expert")
EXPERT_TENSOR_DP = ("expert", "tensor", "dp_0", "dp_1")

NY, NC, NZ, NX = 8, 2, 12, 4
NE = 8
CAP = 9
TOK = 32
NQ = 4
LB = 4
QC = LB * 128
RP = 40
RX = 112
ROWS = NX * RX
ZORDER = (6, 7, 5, 8, 4, 9, 3, 10, 2, 11, 1)
PLUS, MINUS = 0, 1
RS_SLOT = {}
for _s in range(4):
    for _dir, _half, _n in ((PLUS, 0, 4), (MINUS, 1, 4), (PLUS, 1, 3), (MINUS, 0, 3)):
        if _s < _n:
            RS_SLOT[(_dir, _half, _s)] = len(RS_SLOT)
NRS = len(RS_SLOT)


def iota(shape, dim):
    return lax.broadcasted_iota(I32, shape, dim)


def onehot(mask):
    return jnp.where(mask, 1.0, 0.0).astype(BF16)


def dot(a, b, dims=(((1,), (0,)), ((), ())), precision=None):
    return lax.dot_general(a, b, dims, precision=precision, preferred_element_type=F32)


def kernel(
    ids_ref, rin_ref, rwt_ref, grad_ref, down_hbm, hid_hbm,
    wg_ref, hg, rg_ref, ig_ref,
    down, hid, hidp, hidt, image, gcol, relay_r, ids_v, tall,
    chunk, zbuf, xsend, xbuf,
    logit_buf, pg_send, pg_buf, pgx_send, pgx_buf,
    gx_buf, gz_buf,
    rp_send, rc_buf, ry_buf, rz_buf, rx_buf,
    wbuf, dbuf, rsbuf,
    load_sem,
    zs_sem, zr_sem, xs_sem, xr_sem,
    small_s, small_r,
    d_s, d_r, rs_s, rs_r,
):
    y, c = lax.axis_index("dp_0"), lax.axis_index("dp_1")
    z, x = lax.axis_index("expert"), lax.axis_index("tensor")
    oc = 1 - c
    e_lo, e_hi = (z * NX) // 6, (z * NX + NX - 1) // 6
    middle = lax.rem(z, 3) == 1
    sel_hi = lax.rem(z, 3) * (2 - lax.rem(z, 3))
    zpeers = [lax.rem(z + k, NZ) for k in ZORDER]
    xpeers = [lax.rem(x + k, NX) for k in (2, 1, 3)]
    ypeers = [lax.rem(y + k, NY) for k in (4, 5, 3, 6, 2, 7, 1)]
    up, dn = lax.rem(y + 1, NY), lax.rem(y + NY - 1, NY)

    def load(src, dst, i):
        return pltpu.make_async_copy(src, dst, load_sem.at[i])

    load(hid_hbm, hid, 0).start()
    load(down_hbm, down, 1).start()

    def send(src, dst, s_sem, r_sem, **where):
        pltpu.make_async_remote_copy(
            src_ref=src, dst_ref=dst, send_sem=s_sem, recv_sem=r_sem,
            device_id=where, device_id_type=pl.DeviceIdType.MESH,
        ).start()

    def wait(ref, sem):
        pltpu.make_async_copy(ref, ref, sem).wait()

    barrier = pltpu.get_barrier_semaphore()

    def greet(**where):
        pl.semaphore_signal(barrier, inc=1, device_id=where, device_id_type=pl.DeviceIdType.MESH)

    for p in zpeers:
        greet(expert=p)
    for p in xpeers:
        greet(tensor=p)
        greet(tensor=p, dp_1=oc)
    for p in ypeers:
        greet(dp_0=p)
    greet(dp_1=oc)

    for b in range(128 // TOK):
        ids_v[0:2, b * TOK : (b + 1) * TOK] = ids_ref[...]
    sub8 = iota((8, 128), 0)
    ids = [ids_v[0:1, :], ids_v[1:2, :]]
    hit = [sub8 == ids[k] for k in range(2)]
    hits = (jnp.where(hit[0], 1.0, 0.0) + jnp.where(hit[1], 1.0, 0.0)).astype(BF16)
    r128, l128 = iota((128, 128), 0), iota((128, 128), 1)
    tri = onehot((r128 < l128) & (r128 // TOK == l128 // TOK))
    before = dot(hits, tri)
    pos = [jnp.sum(jnp.where(hit[k], before, 0.0), axis=0, keepdims=True).astype(I32) for k in range(2)]
    lane1 = iota((1, 128), 1)
    own_lanes = lane1 // TOK == x
    target = [ids[k] * RP + (lane1 // TOK) * CAP + pos[k] for k in range(2)]
    pack_rows = iota((NE * RP, 128), 0)
    table = onehot((pack_rows == target[0]) | (pack_rows == target[1]))

    def pack(q):
        stack = jnp.concatenate(
            [grad_ref[:, q * QC + b * 128 : q * QC + (b + 1) * 128] for b in range(LB)], axis=0
        )
        packed = dot(table, stack).astype(BF16)
        for e in range(NE):
            chunk[q, e] = packed[e * RP : (e + 1) * RP]

    pack(0)
    logit_buf[x, 0:8] = dot(rwt_ref[:, pl.ds(pl.multiple_of(x * 512, 512), 512)], rin_ref[...], NT)
    info = jnp.zeros((8, 128), F32)
    for row, value in enumerate(ids + pos):
        info = jnp.where(sub8 == row, jnp.where(own_lanes, value.astype(F32), 0.0), info)
    logit_buf[x, 8:16] = info

    pl.semaphore_wait(barrier, len(zpeers) + 2 * len(xpeers) + len(ypeers) + 1)

    for p in xpeers:
        send(logit_buf.at[x], logit_buf.at[x], small_s.at[0], small_r.at[0], tensor=p)

    def z_send(q):
        for p in zpeers:
            lo, hi = (p * NX) // 6, (p * NX + NX - 1) // 6
            send(chunk.at[q, lo], zbuf.at[0, q, z], zs_sem.at[0, q], zr_sem.at[0, q], expert=p)

            @pl.when(lax.rem(p, 3) == 1)
            def _():
                send(chunk.at[q, hi], zbuf.at[1, q, z], zs_sem.at[1, q], zr_sem.at[1, q], expert=p)

    z_send(0)
    for q in range(1, NQ):
        pack(q)
    for q in range(NQ):
        zbuf[0, q, z] = chunk[q, e_lo]
        zbuf[1, q, z] = chunk[q, e_hi]

    others = lambda ref, n: ref.at[0 : n - 1]
    wait(others(logit_buf, NX), small_r.at[0])
    shared = logit_buf[0] + logit_buf[1] + logit_buf[2] + logit_buf[3]
    logits = shared[0:8]
    ids = [shared[8 + k : 9 + k].astype(I32) for k in range(2)]
    pos = [shared[10 + k : 11 + k].astype(I32) for k in range(2)]
    hit = [sub8 == ids[k] for k in range(2)]
    picked = [jnp.sum(jnp.where(hit[k], logits, 0.0), axis=0, keepdims=True) for k in range(2)]
    gate = [jax.nn.sigmoid(picked[0] - picked[1]), jax.nn.sigmoid(picked[1] - picked[0])]
    packed_gate = dot(
        jnp.where(hit[0] & own_lanes, gate[0], 0.0).astype(BF16), onehot(r128 == pos[0]), NT
    ) + dot(jnp.where(hit[1] & own_lanes, gate[1], 0.0).astype(BF16), onehot(r128 == pos[1]), NT)
    pg_send[...] = packed_gate
    pg_buf[z] = packed_gate
    for p in zpeers:
        send(pg_send, pg_buf.at[z], small_s.at[1], small_r.at[1], expert=p)
    z_send(1)
    z_send(2)
    z_send(3)

    rr, kk = iota((RX, NZ * RP), 0), iota((RX, NZ * RP), 1)
    for b in range(LB):
        relay_r[b] = onehot((kk == (rr // CAP) * RP + b * CAP + lax.rem(rr, CAP)) & (rr < NZ * CAP))

    def z_relay(q):
        wait(others(zbuf.at[0, q], NZ), zr_sem.at[0, q])

        @pl.when(middle)
        def _():
            wait(others(zbuf.at[1, q], NZ), zr_sem.at[1, q])

        for cls in range(2):
            rows = zbuf[0 if cls == 0 else sel_hi, q].reshape(NZ * RP, 128)
            for b in range(LB):
                xsend[cls, q, :, b * 128 : (b + 1) * 128] = dot(relay_r[b], rows).astype(BF16)
        for p in xpeers:
            send(xsend.at[p // 2, q], xbuf.at[q, x], xs_sem.at[q], xr_sem.at[q], tensor=p)
        xbuf[q, x] = xsend[x // 2, q]

    load(hid_hbm, hid, 0).wait()
    r1, m1 = iota((ROWS, NX * NZ * CAP), 0), iota((ROWS, NX * NZ * CAP), 1)
    in_col = lax.rem(r1, RX)
    perm = onehot(
        (m1 == ((in_col // CAP) * NX + r1 // RX) * CAP + lax.rem(in_col, CAP)) & (in_col < NZ * CAP)
    )
    hidp[...] = dot(perm, hid[...]).astype(BF16)
    hidt[...] = hidp[...].T

    z_relay(0)

    wait(others(pg_buf, NZ), small_r.at[1])
    sub3 = iota((NZ, 8, 128), 1)
    for cls, e in ((0, e_lo), (1, e_hi)):
        pgx_send[cls] = jnp.zeros((16, 128), F32)
        pgx_send[cls, 0:NZ] = jnp.sum(jnp.where(sub3 == e, pg_buf[...], 0.0), axis=1)
    for p in xpeers:
        send(pgx_send.at[p // 2], pgx_buf.at[x], small_s.at[2], small_r.at[2], tensor=p)
    pgx_buf[x] = pgx_send[x // 2]

    z_relay(1)

    rq, lq = iota((ROWS, 64), 0), iota((ROWS, 64), 1)
    qc = lax.rem(rq, RX)
    column_of = onehot((lq == (rq // RX) * 16 + qc // CAP) & (qc < NZ * CAP))
    rw, lw = iota((ROWS, 128), 0), iota((ROWS, 128), 1)
    own_slot = lw == lax.rem(lax.rem(rw, RX), CAP)

    def make_gates():
        wait(others(pgx_buf, NX), small_r.at[2])
        spread_gate = dot(column_of, pgx_buf[...].reshape(64, 128).astype(BF16))
        column = jnp.sum(jnp.where(own_slot, spread_gate, 0.0), axis=1, keepdims=True)
        gcol[...] = jnp.broadcast_to(column, (ROWS, 128))

    def x_wait(q):
        wait(others(xbuf.at[q], NX), xr_sem.at[q])

    def image_part(q):
        part = dot(xbuf[q].reshape(ROWS, QC), down[:, q * QC : (q + 1) * QC], NT)
        if q == 0:
            image[...] = part
        else:
            image[...] += part

    def weight_part(q):
        rows = xbuf[q].reshape(ROWS, QC).astype(F32)
        gated = (gcol[:, 0:1] * rows).astype(BF16)
        term = dot(hidt[...], gated).astype(BF16)
        for yy in range(NY):
            for cc in range(NC):
                at = (yy * NC + cc) * 80
                wbuf[q, cc, yy] = term[at : at + 80]
        send(wbuf.at[q, oc], dbuf.at[q], d_s.at[q], d_r.at[q], dp_1=oc)

    def cols(half):
        return pl.ds(half * (QC // 2), QC // 2)

    def y_send(q, src, d, half, s):
        slot = RS_SLOT[(d, half, s)]
        send(src, rsbuf.at[q, slot], rs_s.at[q], rs_r.at[q, slot], dp_0=up if d == PLUS else dn)

    def rs_first(q):
        wait(dbuf.at[q], d_r.at[q])
        dbuf[q] = (wbuf[q, c].astype(F32) + dbuf[q].astype(F32)).astype(BF16)
        for d, half, far in ((PLUS, 0, 4), (MINUS, 1, 4), (PLUS, 1, 3), (MINUS, 0, 5)):
            y_send(q, dbuf.at[q, lax.rem(y + far, NY), :, cols(half)], d, half, 0)

    def rs_step(q, s):
        for d, half, n, off in (
            (PLUS, 0, 4, 3 - s), (MINUS, 1, 4, 5 + s), (PLUS, 1, 3, 2 - s), (MINUS, 0, 3, 6 + s),
        ):
            if s >= n:
                continue
            slot = RS_SLOT[(d, half, s)]
            wait(rsbuf.at[q, slot], rs_r.at[q, slot])
            if s == n - 1:
                continue
            block = dbuf[q, lax.rem(y + off, NY), :, half * (QC // 2) : (half + 1) * (QC // 2)]
            rsbuf[q, slot] = (rsbuf[q, slot].astype(F32) + block.astype(F32)).astype(BF16)
            y_send(q, rsbuf.at[q, slot], d, half, s + 1)
        if s == 3:
            for half in range(2):
                lo = half * (QC // 2)
                a = rsbuf[q, RS_SLOT[(PLUS, half, 3 - half)]].astype(F32)
                b = rsbuf[q, RS_SLOT[(MINUS, half, 2 + half)]].astype(F32)
                mine = dbuf[q, y, :, lo : lo + QC // 2].astype(F32)
                wg_ref[:, q * QC + lo : q * QC + lo + QC // 2] = (mine + a + b).astype(BF16)

    make_gates()
    x_wait(0)
    weight_part(0)
    load(down_hbm, down, 1).wait()
    image_part(0)
    z_relay(2)
    rs_first(0)
    x_wait(1)
    weight_part(1)
    image_part(1)
    z_relay(3)
    rs_step(0, 0)
    rs_first(1)
    x_wait(2)
    image_part(2)
    weight_part(2)
    rs_step(0, 1)
    rs_step(1, 0)
    x_wait(3)
    image_part(3)

    slot_sum = jnp.sum(hidp[...].astype(F32) * image[...], axis=1, keepdims=True)
    rt, lt = iota((8, ROWS), 0), iota((8, ROWS), 1)
    back = jnp.where(rt == (x // 2) * sel_hi * NX + lt // RX, 1.0, 0.0)
    own_row = (lw == lax.rem(rw, RX)) & (lw < NZ * CAP)
    gx_buf[x] = dot(back, jnp.where(own_row, slot_sum, 0.0), precision=HIGH)
    for p in xpeers:
        send(gx_buf.at[x], gx_buf.at[x], small_s.at[3], small_r.at[3], tensor=p)

    weight_part(3)
    rs_first(2)

    wait(others(gx_buf, NX), small_r.at[3])
    gz_buf[z] = gx_buf[0] + gx_buf[1] + gx_buf[2] + gx_buf[3]
    for p in zpeers:
        send(gz_buf.at[z], gz_buf.at[z], small_s.at[4], small_r.at[4], expert=p)

    rs_step(0, 2)
    rs_step(1, 1)
    rs_first(3)

    scaled = (gcol[:, 0:1] * image[...]).astype(BF16)
    m2, r2 = iota((NX * NZ * CAP, ROWS), 0), iota((NX * NZ * CAP, ROWS), 1)
    unperm = onehot(r2 == lax.rem(m2 // CAP, NX) * RX + (m2 // (CAP * NX)) * CAP + lax.rem(m2, CAP))
    hg[...] = dot(unperm, scaled).astype(BF16)

    rs_step(2, 0)

    wait(others(gz_buf, NZ), small_r.at[4])
    sums = []
    for p in range(0, NZ, 3):
        sums.append(gz_buf[p] + gz_buf[p + 1])
        sums.append(gz_buf[p + 2] + pltpu.roll(gz_buf[p + 1], 4, 0))
    sums = jnp.concatenate(sums, axis=0)
    r64 = iota((64, 128), 0)
    gate_grad = []
    for k in range(2):
        at_slot = dot(sums, jnp.where(r128 == z * CAP + pos[k], 1.0, 0.0), precision=HIGH)
        mine = r64 == ids[k] * 8 + lane1 // TOK
        gate_grad.append(jnp.sum(jnp.where(mine, at_slot, 0.0), axis=0, keepdims=True))
    mixed = gate[0] * gate_grad[0] + gate[1] * gate_grad[1]
    logit_grad = jnp.where(hit[0], gate[0] * (gate_grad[0] - mixed), 0.0) + jnp.where(
        hit[1], gate[1] * (gate_grad[1] - mixed), 0.0
    )
    router = dot(logit_grad, rin_ref[...].astype(F32), precision=HIGH)
    rp_send[0] = router[:, 0:256]
    rp_send[1] = router[:, 256:512]
    send(rp_send.at[oc], rc_buf, small_s.at[5], small_r.at[5], dp_1=oc)

    rs_step(0, 3)
    rs_step(1, 2)

    wait(rc_buf, small_r.at[5])
    pair = rp_send[c] + rc_buf[...]
    rz_buf[z] = pair
    for p in zpeers:
        send(rz_buf.at[z], rz_buf.at[z], small_s.at[6], small_r.at[6], expert=p)

    rs_step(2, 1)
    rs_step(3, 0)
    tall[...] = jnp.concatenate([logit_grad] * 16, axis=0).T
    own_grad = tall[pl.ds(pl.multiple_of(x * TOK, TOK), TOK), 0:8]
    ig_ref[...] = dot(own_grad, rwt_ref[...].astype(F32), precision=HIGH).astype(BF16)
    rs_step(1, 3)
    rs_step(2, 2)

    wait(others(rz_buf, NZ), small_r.at[6])
    total = rz_buf[0]
    for p in range(1, NZ):
        total = total + rz_buf[p]
    ry_buf[y] = total
    for p in ypeers:
        send(ry_buf.at[y], ry_buf.at[y], small_s.at[7], small_r.at[7], dp_0=p)
    rs_step(3, 1)
    rs_step(2, 3)
    wait(others(ry_buf, NY), small_r.at[7])
    total = ry_buf[0]
    for p in range(1, NY):
        total = total + ry_buf[p]
    here = x * NC + c
    rx_buf[here] = total
    for p in xpeers:
        for cc in (c, oc):
            send(rx_buf.at[here], rx_buf.at[here], small_s.at[8], small_r.at[8], tensor=p, dp_1=cc)
    send(rx_buf.at[here], rx_buf.at[here], small_s.at[8], small_r.at[8], dp_1=oc)
    rs_step(3, 2)
    rs_step(3, 3)
    wait(others(rx_buf, NX * NC), small_r.at[8])
    for i in range(NX * NC):
        rg_ref[:, i * 256 : (i + 1) * 256] = rx_buf[i]

    for q in range(NQ):
        wait(others(zbuf.at[0, q], NZ), zs_sem.at[0, q])

        @pl.when(middle)
        def _():
            wait(zbuf.at[1, q, 0:3], zs_sem.at[1, q])

        @pl.when(jnp.logical_not(middle))
        def _():
            wait(zbuf.at[1, q, 0:4], zs_sem.at[1, q])

        wait(others(xbuf.at[q], NX), xs_sem.at[q])
        wait(dbuf.at[q], d_s.at[q])
        wait(rsbuf.at[q], rs_s.at[q])
    for i, (buf, n) in enumerate(
        ((logit_buf, NX), (pg_buf, NZ), (pgx_buf, NX), (gx_buf, NX), (gz_buf, NZ))
    ):
        wait(others(buf, n), small_s.at[i])
    wait(rc_buf, small_s.at[5])
    wait(others(rz_buf, NZ), small_s.at[6])
    wait(others(ry_buf, NY), small_s.at[7])
    wait(others(rx_buf, NX * NC), small_s.at[8])


def write_out(wg, hg, rg, ig, wg_out, hg_out, rg_out, ig_out, sem):
    copies = [
        pltpu.make_async_copy(src, dst, sem.at[i])
        for i, (src, dst) in enumerate(((hg, hg_out), (wg, wg_out), (ig, ig_out), (rg, rg_out)))
    ]
    for copy in copies:
        copy.start()
    for copy in copies:
        copy.wait()


def per_device(router_input, router_weight, expert_ids, down_weight, hidden, grad_output):
    ids = expert_ids.T
    rwt = router_weight.T
    slots, units = hidden.shape[1], hidden.shape[2]
    width = grad_output.shape[1]
    vmem = pl.BlockSpec(memory_space=pltpu.VMEM)
    hbm = pl.BlockSpec(memory_space=pl.ANY)
    V = pltpu.VMEM
    dma = pltpu.SemaphoreType.DMA
    results = (
        ((units // (NY * NC), width), BF16),
        ((slots, units), BF16),
        ((8, width), F32),
        ((TOK, width), BF16),
    )
    inner = pl.pallas_call(
        kernel,
        out_shape=tuple(V(shape, kind) for shape, kind in results),
        in_specs=[vmem, vmem, vmem, vmem, hbm, hbm],
        out_specs=(vmem, vmem, vmem, vmem),
        scratch_shapes=[
            V((units, width), BF16),
            V((slots, units), BF16),
            V((ROWS, units), BF16),
            V((units, ROWS), BF16),
            V((ROWS, units), F32),
            V((ROWS, 128), F32),
            V((LB, RX, NZ * RP), BF16),
            V((8, 128), I32),
            V((128, 128), F32),
            V((NQ, NE, RP, 128), BF16),
            V((2, NQ, NZ, RP, 128), BF16),
            V((2, NQ, RX, QC), BF16),
            V((NQ, NX, RX, QC), BF16),
            V((NX, 16, 128), F32),
            V((8, 128), F32),
            V((NZ, 8, 128), F32),
            V((2, 16, 128), F32),
            V((NX, 16, 128), F32),
            V((NX, 8, 128), F32),
            V((NZ, 8, 128), F32),
            V((2, 8, 256), F32),
            V((8, 256), F32),
            V((NY, 8, 256), F32),
            V((NZ, 8, 256), F32),
            V((NX * NC, 8, 256), F32),
            V((NQ, NC, NY, 80, QC), BF16),
            V((NQ, NY, 80, QC), BF16),
            V((NQ, NRS, 80, QC // 2), BF16),
            dma((2,)),
            dma((2, NQ)), dma((2, NQ)), dma((NQ,)), dma((NQ,)),
            dma((9,)), dma((9,)),
            dma((NQ,)), dma((NQ,)), dma((NQ,)), dma((NQ, NRS)),
        ],
        compiler_params=pltpu.CompilerParams(
            collective_id=0, has_side_effects=True, vmem_limit_bytes=60 * 1024 * 1024
        ),
    )(ids, router_input, rwt, grad_output, down_weight, hidden[0])
    weight_grad, hidden_grad, router, input_grad = pl.pallas_call(
        write_out,
        out_shape=tuple(jax.ShapeDtypeStruct(shape, kind) for shape, kind in results),
        in_specs=[vmem] * 4,
        out_specs=(hbm,) * 4,
        scratch_shapes=[dma((4,))],
        compiler_params=pltpu.CompilerParams(vmem_limit_bytes=1024 * 1024),
    )(*inner)
    return weight_grad, hidden_grad[None], router.T, input_grad


def solution(mesh):
    finer = Mesh(
        mesh.devices.reshape(NY, NC, mesh.shape["expert"], mesh.shape["tensor"]),
        ("dp_0", "dp_1", "expert", "tensor"),
    )
    placed = (
        P(DP_EXPERT, "tensor"),
        P(),
        P(DP_EXPERT_TENSOR, None),
        P(("expert", "tensor"), None),
        P(DP, None, ("expert", "tensor")),
        P(DP_EXPERT_TENSOR, None),
    )
    return jax.shard_map(
        per_device,
        mesh=finer,
        in_specs=placed,
        out_specs=(
            P(EXPERT_TENSOR_DP, None),
            P(DP, None, ("expert", "tensor")),
            P(),
            P(DP_EXPERT_TENSOR, None),
        ),
        check_vma=False,
    )
```

```python
import functools

import jax
import jax.numpy as jnp
from jax import lax
from jax.experimental import pallas as pl
from jax.experimental.pallas import tpu as pltpu
from jax.sharding import Mesh
from jax.sharding import PartitionSpec as P

F32 = jnp.float32
BF16 = jnp.bfloat16
I32 = jnp.int32
HIGH = lax.Precision.HIGHEST
NT = (((1,), (1,)), ((), ()))

DP = ("dp_0", "dp_1")
DP_EXPERT_TENSOR = ("dp_0", "dp_1", "expert", "tensor")
DP_EXPERT = ("dp_0", "dp_1", "expert")
EXPERT_TENSOR_DP = ("expert", "tensor", "dp_0", "dp_1")

NY, NC, NZ, NX = 8, 2, 12, 4
NE = 8
CAP = 9
TOK = 32
NQ = 4
LB = 4
QC = LB * 128
RP = 40
RX = 112
ROWS = NX * RX
HALF = NZ // 2
RH = RX // 2
ZORDER = (6, 7, 5, 8, 4, 9, 3, 10, 2, 11, 1)
PLUS, MINUS = 0, 1
RS_SLOT = {}
for _s in range(4):
    for _dir, _half, _n in ((PLUS, 0, 4), (MINUS, 1, 4), (PLUS, 1, 3), (MINUS, 0, 3)):
        if _s < _n:
            RS_SLOT[(_dir, _half, _s)] = len(RS_SLOT)
NRS = len(RS_SLOT)


def iota(shape, dim):
    return lax.broadcasted_iota(I32, shape, dim)


def onehot(mask):
    return jnp.where(mask, 1.0, 0.0).astype(BF16)


def dot(a, b, dims=(((1,), (0,)), ((), ())), precision=None):
    return lax.dot_general(a, b, dims, precision=precision, preferred_element_type=F32)


def kernel(
    ids_ref, rin_ref, rwt_ref, grad_ref, down_hbm, hid_hbm,
    wg_ref, hg, rg_ref, ig_ref,
    down, hid, hidp, hidt, image, gcol, relay_r, ids_v, tall,
    chunk, zbuf, xsend, xbuf,
    logit_buf, pg_send, pg_buf, pgx_send, pgx_buf,
    gx_buf, gz_buf,
    rp_send, rc_buf, ry_buf, rz_buf, rx_buf,
    wbuf, dbuf, rsbuf,
    load_sem,
    zs_sem, zr_sem, fs_sem, fr_sem, xs_sem, xr_sem,
    small_s, small_r,
    d_s, d_r, rs_s, rs_r,
):
    y, c = lax.axis_index("dp_0"), lax.axis_index("dp_1")
    z, x = lax.axis_index("expert"), lax.axis_index("tensor")
    oc = 1 - c
    e_lo, e_hi = (z * NX) // 6, (z * NX + NX - 1) // 6
    middle = lax.rem(z, 3) == 1
    third = lax.rem(z, 3)
    sel_hi = third * (2 - third)
    zpeers = [lax.rem(z + k, NZ) for k in ZORDER]
    xpeers = [lax.rem(x + k, NX) for k in (2, 1, 3)]
    ypeers = [lax.rem(y + k, NY) for k in (4, 5, 3, 6, 2, 7, 1)]
    up, dn = lax.rem(y + 1, NY), lax.rem(y + NY - 1, NY)

    def load(src, dst, i):
        return pltpu.make_async_copy(src, dst, load_sem.at[i])

    load(hid_hbm, hid, 0).start()
    load(down_hbm, down, 1).start()

    def send(src, dst, s_sem, r_sem, **where):
        pltpu.make_async_remote_copy(
            src_ref=src, dst_ref=dst, send_sem=s_sem, recv_sem=r_sem,
            device_id=where, device_id_type=pl.DeviceIdType.MESH,
        ).start()

    def wait(ref, sem):
        pltpu.make_async_copy(ref, ref, sem).wait()

    barrier = pltpu.get_barrier_semaphore()

    def greet(**where):
        pl.semaphore_signal(barrier, inc=1, device_id=where, device_id_type=pl.DeviceIdType.MESH)

    for p in zpeers:
        greet(expert=p)
    for p in xpeers:
        greet(tensor=p)
        greet(tensor=p, dp_1=oc)
    for p in ypeers:
        greet(dp_0=p)
    greet(dp_1=oc)

    for b in range(128 // TOK):
        ids_v[0:2, b * TOK : (b + 1) * TOK] = ids_ref[...]
    sub8 = iota((8, 128), 0)
    ids = [ids_v[0:1, :], ids_v[1:2, :]]
    hit = [sub8 == ids[k] for k in range(2)]
    hits = (jnp.where(hit[0], 1.0, 0.0) + jnp.where(hit[1], 1.0, 0.0)).astype(BF16)
    r128, l128 = iota((128, 128), 0), iota((128, 128), 1)
    tri = onehot((r128 < l128) & (r128 // TOK == l128 // TOK))
    before = dot(hits, tri)
    pos = [jnp.sum(jnp.where(hit[k], before, 0.0), axis=0, keepdims=True).astype(I32) for k in range(2)]
    lane1 = iota((1, 128), 1)
    own_lanes = lane1 // TOK == x
    target = [ids[k] * RP + (lane1 // TOK) * CAP + pos[k] for k in range(2)]
    pack_rows = iota((NE * RP, 128), 0)
    table = onehot((pack_rows == target[0]) | (pack_rows == target[1]))

    def pack(q):
        stack = jnp.concatenate(
            [grad_ref[:, q * QC + b * 128 : q * QC + (b + 1) * 128] for b in range(LB)], axis=0
        )
        packed = dot(table, stack).astype(BF16)
        for e in range(NE):
            chunk[q, e] = packed[e * RP : (e + 1) * RP]

    pack(0)
    logit_buf[x, 0:8] = dot(rwt_ref[:, pl.ds(pl.multiple_of(x * 512, 512), 512)], rin_ref[...], NT)
    info = jnp.zeros((8, 128), F32)
    for row, value in enumerate(ids + pos):
        info = jnp.where(sub8 == row, jnp.where(own_lanes, value.astype(F32), 0.0), info)
    logit_buf[x, 8:16] = info

    pl.semaphore_wait(barrier, len(zpeers) + 2 * len(xpeers) + len(ypeers) + 1)

    for p in xpeers:
        send(logit_buf.at[x], logit_buf.at[x], small_s.at[0], small_r.at[0], tensor=p)

    def z_send(q):
        for d in range(HALF - 1, 0, -1):
            above, below = lax.rem(z + d, NZ), lax.rem(z + NZ - d, NZ)
            ra, rb = lax.rem(above, 3), lax.rem(below, 3)

            @pl.when(ra < 2)
            def _():
                send(
                    chunk.at[q, above // 3 * 2 + ra], zbuf.at[ra, q, d],
                    zs_sem.at[q], zr_sem.at[ra, q], expert=above,
                )

            @pl.when(rb > 0)
            def _():
                send(
                    chunk.at[q, below // 3 * 2 + rb - 1], zbuf.at[0, q, d],
                    zs_sem.at[q], zr_sem.at[0, q], expert=below,
                )

    def z_own(q):
        zbuf[0, q, 0] = chunk[q, e_lo]
        zbuf[1, q, 0] = chunk[q, e_hi]

    def z_forward(q):
        near, far = pl.ds(0, HALF), pl.ds(HALF, HALF)
        wait(zbuf.at[0, q, 1:HALF], zr_sem.at[0, q])
        cls = third // 2
        neighbour = jnp.where(third == 0, z + 1, z - 1)
        send(
            zbuf.at[0, q, near], zbuf.at[cls, q, far], fs_sem.at[0, q], fr_sem.at[cls, q], expert=neighbour
        )

        @pl.when(middle)
        def _():
            wait(zbuf.at[1, q, 1:HALF], zr_sem.at[1, q])
            send(
                zbuf.at[1, q, near], zbuf.at[0, q, far], fs_sem.at[1, q], fr_sem.at[0, q], expert=z + 1
            )

    z_own(0)
    z_send(0)
    for q in range(1, NQ):
        pack(q)
        z_own(q)

    rr, kk = iota((RH, HALF * RP), 0), iota((RH, HALF * RP), 1)
    for b in range(LB):
        relay_r[b] = onehot((kk == (rr // CAP) * RP + b * CAP + lax.rem(rr, CAP)) & (rr < HALF * CAP))
    side = jnp.where((third == 0) | ((x // 2) * sel_hi == 1), -1, 1)

    def place_of(row):
        col, in_col = row // RX, lax.rem(row, RX)
        in_half = lax.rem(in_col, RH)
        dist, slot = in_half // CAP, lax.rem(in_half, CAP)
        source = jnp.where(in_col < RH, z + side * dist, z - side - side * dist)
        return col, lax.rem(source + 2 * NZ, NZ), slot, in_half < HALF * CAP

    load(hid_hbm, hid, 0).wait()
    col, source, slot, used = place_of(iota((ROWS, NX * NZ * CAP), 0))
    perm = onehot((iota((ROWS, NX * NZ * CAP), 1) == (source * NX + col) * CAP + slot) & used)
    hidp[...] = dot(perm, hid[...]).astype(BF16)
    hidt[...] = hidp[...].T

    others = lambda ref, n: ref.at[0 : n - 1]
    wait(others(logit_buf, NX), small_r.at[0])
    shared = logit_buf[0] + logit_buf[1] + logit_buf[2] + logit_buf[3]
    logits = shared[0:8]
    ids = [shared[8 + k : 9 + k].astype(I32) for k in range(2)]
    pos = [shared[10 + k : 11 + k].astype(I32) for k in range(2)]
    hit = [sub8 == ids[k] for k in range(2)]
    picked = [jnp.sum(jnp.where(hit[k], logits, 0.0), axis=0, keepdims=True) for k in range(2)]
    gate = [jax.nn.sigmoid(picked[0] - picked[1]), jax.nn.sigmoid(picked[1] - picked[0])]
    packed_gate = dot(
        jnp.where(hit[0] & own_lanes, gate[0], 0.0).astype(BF16), onehot(r128 == pos[0]), NT
    ) + dot(jnp.where(hit[1] & own_lanes, gate[1], 0.0).astype(BF16), onehot(r128 == pos[1]), NT)
    pg_send[...] = packed_gate
    pg_buf[z] = packed_gate
    for p in zpeers:
        send(pg_send, pg_buf.at[z], small_s.at[1], small_r.at[1], expert=p)
    z_send(1)

    def z_relay(q, half):
        if half:
            wait(zbuf.at[0, q, HALF:NZ], fr_sem.at[0, q])

            @pl.when(middle)
            def _():
                wait(zbuf.at[1, q, HALF:NZ], fr_sem.at[1, q])

        for cls in range(2):
            at = 0 if cls == 0 else sel_hi
            rows = zbuf[at, q, half * HALF : (half + 1) * HALF].reshape(HALF * RP, 128)
            for b in range(LB):
                xsend[cls, q, half, :, b * 128 : (b + 1) * 128] = dot(relay_r[b], rows).astype(BF16)
        for p in xpeers:
            send(
                xsend.at[p // 2, q, half], xbuf.at[q, x, half], xs_sem.at[q], xr_sem.at[q], tensor=p
            )
        xbuf[q, x, half] = xsend[x // 2, q, half]

    z_forward(0)
    z_relay(0, 0)
    z_send(2)

    wait(others(pg_buf, NZ), small_r.at[1])
    sub3 = iota((NZ, 8, 128), 1)
    for cls, e in ((0, e_lo), (1, e_hi)):
        pgx_send[cls] = jnp.zeros((16, 128), F32)
        pgx_send[cls, 0:NZ] = jnp.sum(jnp.where(sub3 == e, pg_buf[...], 0.0), axis=1)
    for p in xpeers:
        send(pgx_send.at[p // 2], pgx_buf.at[x], small_s.at[2], small_r.at[2], tensor=p)
    pgx_buf[x] = pgx_send[x // 2]

    z_forward(1)
    z_relay(1, 0)
    z_relay(0, 1)
    z_send(3)
    z_forward(2)
    z_relay(2, 0)
    z_relay(1, 1)

    col, source, slot, used = place_of(iota((ROWS, 64), 0))
    column_of = onehot((iota((ROWS, 64), 1) == col * 16 + source) & used)
    col, source, slot, used = place_of(iota((ROWS, 128), 0))
    own_slot = iota((ROWS, 128), 1) == slot
    own_row = (iota((ROWS, 128), 1) == source * CAP + slot) & used

    def make_gates():
        wait(others(pgx_buf, NX), small_r.at[2])
        spread_gate = dot(column_of, pgx_buf[...].reshape(64, 128).astype(BF16))
        column = jnp.sum(jnp.where(own_slot, spread_gate, 0.0), axis=1, keepdims=True)
        gcol[...] = jnp.broadcast_to(column, (ROWS, 128))

    def x_wait(q):
        wait(others(xbuf.at[q], NX), xr_sem.at[q])

    def image_part(q):
        part = dot(xbuf[q].reshape(ROWS, QC), down[:, q * QC : (q + 1) * QC], NT)
        if q == 0:
            image[...] = part
        else:
            image[...] += part

    def weight_part(q):
        rows = xbuf[q].reshape(ROWS, QC).astype(F32)
        gated = (gcol[:, 0:1] * rows).astype(BF16)
        term = dot(hidt[...], gated).astype(BF16)
        for yy in range(NY):
            for cc in range(NC):
                at = (yy * NC + cc) * 80
                wbuf[q, cc, yy] = term[at : at + 80]
        send(wbuf.at[q, oc], dbuf.at[q], d_s.at[q], d_r.at[q], dp_1=oc)

    def cols(half):
        return pl.ds(half * (QC // 2), QC // 2)

    def y_send(q, src, d, half, s):
        slot = RS_SLOT[(d, half, s)]
        send(src, rsbuf.at[q, slot], rs_s.at[q], rs_r.at[q, slot], dp_0=up if d == PLUS else dn)

    def rs_first(q):
        wait(dbuf.at[q], d_r.at[q])
        dbuf[q] = (wbuf[q, c].astype(F32) + dbuf[q].astype(F32)).astype(BF16)
        for d, half, far in ((PLUS, 0, 4), (MINUS, 1, 4), (PLUS, 1, 3), (MINUS, 0, 5)):
            y_send(q, dbuf.at[q, lax.rem(y + far, NY), :, cols(half)], d, half, 0)

    def rs_step(q, s):
        for d, half, n, off in (
            (PLUS, 0, 4, 3 - s), (MINUS, 1, 4, 5 + s), (PLUS, 1, 3, 2 - s), (MINUS, 0, 3, 6 + s),
        ):
            if s >= n:
                continue
            slot = RS_SLOT[(d, half, s)]
            wait(rsbuf.at[q, slot], rs_r.at[q, slot])
            if s == n - 1:
                continue
            block = dbuf[q, lax.rem(y + off, NY), :, half * (QC // 2) : (half + 1) * (QC // 2)]
            rsbuf[q, slot] = (rsbuf[q, slot].astype(F32) + block.astype(F32)).astype(BF16)
            y_send(q, rsbuf.at[q, slot], d, half, s + 1)
        if s == 3:
            for half in range(2):
                lo = half * (QC // 2)
                a = rsbuf[q, RS_SLOT[(PLUS, half, 3 - half)]].astype(F32)
                b = rsbuf[q, RS_SLOT[(MINUS, half, 2 + half)]].astype(F32)
                mine = dbuf[q, y, :, lo : lo + QC // 2].astype(F32)
                wg_ref[:, q * QC + lo : q * QC + lo + QC // 2] = (mine + a + b).astype(BF16)

    make_gates()
    x_wait(0)
    weight_part(0)
    z_forward(3)
    z_relay(3, 0)
    z_relay(2, 1)
    load(down_hbm, down, 1).wait()
    image_part(0)
    rs_first(0)
    z_relay(3, 1)
    x_wait(1)
    weight_part(1)
    image_part(1)
    rs_step(0, 0)
    rs_first(1)
    x_wait(2)
    weight_part(2)
    image_part(2)
    rs_step(0, 1)
    rs_first(2)
    rs_step(1, 0)
    x_wait(3)
    image_part(3)

    slot_sum = jnp.sum(hidp[...].astype(F32) * image[...], axis=1, keepdims=True)
    rt, lt = iota((8, ROWS), 0), iota((8, ROWS), 1)
    back = jnp.where(rt == (x // 2) * sel_hi * NX + lt // RX, 1.0, 0.0)
    gx_buf[x] = dot(back, jnp.where(own_row, slot_sum, 0.0), precision=HIGH)
    for p in xpeers:
        send(gx_buf.at[x], gx_buf.at[x], small_s.at[3], small_r.at[3], tensor=p)

    weight_part(3)
    rs_step(0, 2)

    wait(others(gx_buf, NX), small_r.at[3])
    gz_buf[z] = gx_buf[0] + gx_buf[1] + gx_buf[2] + gx_buf[3]
    for p in zpeers:
        send(gz_buf.at[z], gz_buf.at[z], small_s.at[4], small_r.at[4], expert=p)

    rs_first(3)
    rs_step(1, 1)
    rs_step(2, 0)
    rs_step(0, 3)

    scaled = (gcol[:, 0:1] * image[...]).astype(BF16)
    col, source, slot, used = place_of(iota((NX * NZ * CAP, ROWS), 1))
    unperm = onehot((iota((NX * NZ * CAP, ROWS), 0) == (source * NX + col) * CAP + slot) & used)
    hg[...] = dot(unperm, scaled).astype(BF16)

    rs_step(3, 0)
    rs_step(1, 2)

    wait(others(gz_buf, NZ), small_r.at[4])
    sums = []
    for p in range(0, NZ, 3):
        sums.append(gz_buf[p] + gz_buf[p + 1])
        sums.append(gz_buf[p + 2] + pltpu.roll(gz_buf[p + 1], 4, 0))
    sums = jnp.concatenate(sums, axis=0)
    r64 = iota((64, 128), 0)
    gate_grad = []
    for k in range(2):
        at_slot = dot(sums, jnp.where(r128 == z * CAP + pos[k], 1.0, 0.0), precision=HIGH)
        mine = r64 == ids[k] * 8 + lane1 // TOK
        gate_grad.append(jnp.sum(jnp.where(mine, at_slot, 0.0), axis=0, keepdims=True))
    mixed = gate[0] * gate_grad[0] + gate[1] * gate_grad[1]
    logit_grad = jnp.where(hit[0], gate[0] * (gate_grad[0] - mixed), 0.0) + jnp.where(
        hit[1], gate[1] * (gate_grad[1] - mixed), 0.0
    )
    router = dot(logit_grad, rin_ref[...].astype(F32), precision=HIGH)
    rp_send[0] = router[:, 0:256]
    rp_send[1] = router[:, 256:512]
    send(rp_send.at[oc], rc_buf, small_s.at[5], small_r.at[5], dp_1=oc)

    rs_step(2, 1)
    wait(rc_buf, small_r.at[5])
    pair = rp_send[c] + rc_buf[...]
    rz_buf[z] = pair
    for p in zpeers:
        send(rz_buf.at[z], rz_buf.at[z], small_s.at[6], small_r.at[6], expert=p)

    rs_step(3, 1)
    rs_step(1, 3)
    rs_step(2, 2)
    tall[...] = jnp.concatenate([logit_grad] * 16, axis=0).T
    own_grad = tall[pl.ds(pl.multiple_of(x * TOK, TOK), TOK), 0:8]
    ig_ref[...] = dot(own_grad, rwt_ref[...].astype(F32), precision=HIGH).astype(BF16)
    rs_step(3, 2)
    rs_step(2, 3)
    wait(others(rz_buf, NZ), small_r.at[6])
    total = rz_buf[0]
    for p in range(1, NZ):
        total = total + rz_buf[p]
    ry_buf[y] = total
    for p in ypeers:
        send(ry_buf.at[y], ry_buf.at[y], small_s.at[7], small_r.at[7], dp_0=p)
    rs_step(3, 3)
    wait(others(ry_buf, NY), small_r.at[7])
    total = ry_buf[0]
    for p in range(1, NY):
        total = total + ry_buf[p]
    here = x * NC + c
    rx_buf[here] = total
    for p in xpeers:
        for cc in (c, oc):
            send(rx_buf.at[here], rx_buf.at[here], small_s.at[8], small_r.at[8], tensor=p, dp_1=cc)
    send(rx_buf.at[here], rx_buf.at[here], small_s.at[8], small_r.at[8], dp_1=oc)
    wait(others(rx_buf, NX * NC), small_r.at[8])
    for i in range(NX * NC):
        rg_ref[:, i * 256 : (i + 1) * 256] = rx_buf[i]

    for q in range(NQ):
        wait(zbuf.at[0, q, 0:HALF], fs_sem.at[0, q])

        @pl.when(middle)
        def _():
            wait(zbuf.at[0, q, 0 : NE - 2], zs_sem.at[q])
            wait(zbuf.at[1, q, 0:HALF], fs_sem.at[1, q])

        @pl.when(jnp.logical_not(middle))
        def _():
            wait(zbuf.at[0, q, 0 : NE - 1], zs_sem.at[q])

        wait(others(xbuf.at[q], NX), xs_sem.at[q])
        wait(dbuf.at[q], d_s.at[q])
        wait(rsbuf.at[q], rs_s.at[q])
    for i, (buf, n) in enumerate(
        ((logit_buf, NX), (pg_buf, NZ), (pgx_buf, NX), (gx_buf, NX), (gz_buf, NZ))
    ):
        wait(others(buf, n), small_s.at[i])
    wait(rc_buf, small_s.at[5])
    wait(others(rz_buf, NZ), small_s.at[6])
    wait(others(ry_buf, NY), small_s.at[7])
    wait(others(rx_buf, NX * NC), small_s.at[8])


def write_out(wg, hg, rg, ig, wg_out, hg_out, rg_out, ig_out, sem):
    copies = [
        pltpu.make_async_copy(src, dst, sem.at[i])
        for i, (src, dst) in enumerate(((hg, hg_out), (wg, wg_out), (ig, ig_out), (rg, rg_out)))
    ]
    for copy in copies:
        copy.start()
    for copy in copies:
        copy.wait()


def per_device(router_input, router_weight, expert_ids, down_weight, hidden, grad_output):
    ids = expert_ids.T
    rwt = router_weight.T
    slots, units = hidden.shape[1], hidden.shape[2]
    width = grad_output.shape[1]
    vmem = pl.BlockSpec(memory_space=pltpu.VMEM)
    hbm = pl.BlockSpec(memory_space=pl.ANY)
    V = pltpu.VMEM
    dma = pltpu.SemaphoreType.DMA
    results = (
        ((units // (NY * NC), width), BF16),
        ((slots, units), BF16),
        ((8, width), F32),
        ((TOK, width), BF16),
    )
    inner = pl.pallas_call(
        kernel,
        out_shape=tuple(V(shape, kind) for shape, kind in results),
        in_specs=[vmem, vmem, vmem, vmem, hbm, hbm],
        out_specs=(vmem, vmem, vmem, vmem),
        scratch_shapes=[
            V((units, width), BF16),
            V((slots, units), BF16),
            V((ROWS, units), BF16),
            V((units, ROWS), BF16),
            V((ROWS, units), F32),
            V((ROWS, 128), F32),
            V((LB, RH, HALF * RP), BF16),
            V((8, 128), I32),
            V((128, 128), F32),
            V((NQ, NE, RP, 128), BF16),
            V((2, NQ, NZ, RP, 128), BF16),
            V((2, NQ, 2, RH, QC), BF16),
            V((NQ, NX, 2, RH, QC), BF16),
            V((NX, 16, 128), F32),
            V((8, 128), F32),
            V((NZ, 8, 128), F32),
            V((2, 16, 128), F32),
            V((NX, 16, 128), F32),
            V((NX, 8, 128), F32),
            V((NZ, 8, 128), F32),
            V((2, 8, 256), F32),
            V((8, 256), F32),
            V((NY, 8, 256), F32),
            V((NZ, 8, 256), F32),
            V((NX * NC, 8, 256), F32),
            V((NQ, NC, NY, 80, QC), BF16),
            V((NQ, NY, 80, QC), BF16),
            V((NQ, NRS, 80, QC // 2), BF16),
            dma((2,)),
            dma((NQ,)), dma((2, NQ)), dma((2, NQ)), dma((2, NQ)),
            dma((NQ,)), dma((NQ,)),
            dma((9,)), dma((9,)),
            dma((NQ,)), dma((NQ,)), dma((NQ,)), dma((NQ, NRS)),
        ],
        compiler_params=pltpu.CompilerParams(
            collective_id=0, has_side_effects=True, vmem_limit_bytes=60 * 1024 * 1024
        ),
    )(ids, router_input, rwt, grad_output, down_weight, hidden[0])
    weight_grad, hidden_grad, router, input_grad = pl.pallas_call(
        write_out,
        out_shape=tuple(jax.ShapeDtypeStruct(shape, kind) for shape, kind in results),
        in_specs=[vmem] * 4,
        out_specs=(hbm,) * 4,
        scratch_shapes=[dma((4,))],
        compiler_params=pltpu.CompilerParams(vmem_limit_bytes=1024 * 1024),
    )(*inner)
    return weight_grad, hidden_grad[None], router.T, input_grad


def solution(mesh):
    finer = Mesh(
        mesh.devices.reshape(NY, NC, mesh.shape["expert"], mesh.shape["tensor"]),
        ("dp_0", "dp_1", "expert", "tensor"),
    )
    placed = (
        P(DP_EXPERT, "tensor"),
        P(),
        P(DP_EXPERT_TENSOR, None),
        P(("expert", "tensor"), None),
        P(DP, None, ("expert", "tensor")),
        P(DP_EXPERT_TENSOR, None),
    )
    return jax.shard_map(
        per_device,
        mesh=finer,
        in_specs=placed,
        out_specs=(
            P(EXPERT_TENSOR_DP, None),
            P(DP, None, ("expert", "tensor")),
            P(),
            P(DP_EXPERT_TENSOR, None),
        ),
        check_vma=False,
    )
```

```python
import functools

import jax
import jax.numpy as jnp
from jax import lax
from jax.experimental import pallas as pl
from jax.experimental.pallas import tpu as pltpu
from jax.sharding import Mesh
from jax.sharding import PartitionSpec as P

F32 = jnp.float32
BF16 = jnp.bfloat16
I32 = jnp.int32
HIGH = lax.Precision.HIGHEST
NT = (((1,), (1,)), ((), ()))

DP = ("dp_0", "dp_1")
DP_EXPERT_TENSOR = ("dp_0", "dp_1", "expert", "tensor")
DP_EXPERT = ("dp_0", "dp_1", "expert")
EXPERT_TENSOR_DP = ("expert", "tensor", "dp_0", "dp_1")

NY, NC, NZ, NX = 8, 2, 12, 4
NE = 8
CAP = 9
TOK = 32
NQ = 4
LB = 4
QC = LB * 128
RP = 40
RX = 112
ROWS = NX * RX
HALF = NZ // 2
RH = RX // 2
ZORDER = (6, 7, 5, 8, 4, 9, 3, 10, 2, 11, 1)
PLUS, MINUS = 0, 1
RS_SLOT = {}
for _s in range(4):
    for _dir, _half, _n in ((PLUS, 0, 4), (MINUS, 1, 4), (PLUS, 1, 3), (MINUS, 0, 3)):
        if _s < _n:
            RS_SLOT[(_dir, _half, _s)] = len(RS_SLOT)
NRS = len(RS_SLOT)


def iota(shape, dim):
    return lax.broadcasted_iota(I32, shape, dim)


def onehot(mask):
    return jnp.where(mask, 1.0, 0.0).astype(BF16)


def dot(a, b, dims=(((1,), (0,)), ((), ())), precision=None):
    return lax.dot_general(a, b, dims, precision=precision, preferred_element_type=F32)


def kernel(
    ids_ref, rin_ref, rwt_ref, grad_ref, down_hbm, hid_hbm,
    wg_ref, hg, rg_ref, ig_ref,
    down, hid, hidp, hidt, image, gcol, relay_r, ids_v, tall,
    chunk, zbuf, xsend, xbuf,
    logit_buf, pg_send, pg_buf, pgx_send, pgx_buf,
    gx_buf, gz_buf,
    rp_send, rc_buf, ry_buf, rz_buf, rx_buf,
    wbuf, dbuf, rsbuf,
    load_sem,
    zs_sem, zr_sem, fs_sem, fr_sem, xs_sem, xr_sem,
    small_s, small_r,
    d_s, d_r, rs_s, rs_r,
):
    y, c = lax.axis_index("dp_0"), lax.axis_index("dp_1")
    z, x = lax.axis_index("expert"), lax.axis_index("tensor")
    oc = 1 - c
    e_lo, e_hi = (z * NX) // 6, (z * NX + NX - 1) // 6
    middle = lax.rem(z, 3) == 1
    third = lax.rem(z, 3)
    sel_hi = third * (2 - third)
    zpeers = [lax.rem(z + k, NZ) for k in ZORDER]
    xpeers = [lax.rem(x + k, NX) for k in (2, 1, 3)]
    ypeers = [lax.rem(y + k, NY) for k in (4, 5, 3, 6, 2, 7, 1)]
    up, dn = lax.rem(y + 1, NY), lax.rem(y + NY - 1, NY)

    def load(src, dst, i):
        return pltpu.make_async_copy(src, dst, load_sem.at[i])

    load(hid_hbm, hid, 0).start()
    load(down_hbm, down, 1).start()

    def send(src, dst, s_sem, r_sem, **where):
        pltpu.make_async_remote_copy(
            src_ref=src, dst_ref=dst, send_sem=s_sem, recv_sem=r_sem,
            device_id=where, device_id_type=pl.DeviceIdType.MESH,
        ).start()

    def wait(ref, sem):
        pltpu.make_async_copy(ref, ref, sem).wait()

    barrier = pltpu.get_barrier_semaphore()

    def greet(**where):
        pl.semaphore_signal(barrier, inc=1, device_id=where, device_id_type=pl.DeviceIdType.MESH)

    for p in zpeers:
        greet(expert=p)
    for p in xpeers:
        greet(tensor=p)
        greet(tensor=p, dp_1=oc)
    for p in ypeers:
        greet(dp_0=p)
    greet(dp_1=oc)

    for b in range(128 // TOK):
        ids_v[0:2, b * TOK : (b + 1) * TOK] = ids_ref[...]
    sub8 = iota((8, 128), 0)
    ids = [ids_v[0:1, :], ids_v[1:2, :]]
    hit = [sub8 == ids[k] for k in range(2)]
    hits = (jnp.where(hit[0], 1.0, 0.0) + jnp.where(hit[1], 1.0, 0.0)).astype(BF16)
    r128, l128 = iota((128, 128), 0), iota((128, 128), 1)
    tri = onehot((r128 < l128) & (r128 // TOK == l128 // TOK))
    before = dot(hits, tri)
    pos = [jnp.sum(jnp.where(hit[k], before, 0.0), axis=0, keepdims=True).astype(I32) for k in range(2)]
    lane1 = iota((1, 128), 1)
    own_lanes = lane1 // TOK == x
    target = [ids[k] * RP + (lane1 // TOK) * CAP + pos[k] for k in range(2)]
    pack_rows = iota((NE * RP, 128), 0)
    table = onehot((pack_rows == target[0]) | (pack_rows == target[1]))

    def pack(q):
        stack = jnp.concatenate(
            [grad_ref[:, q * QC + b * 128 : q * QC + (b + 1) * 128] for b in range(LB)], axis=0
        )
        packed = dot(table, stack).astype(BF16)
        for e in range(NE):
            chunk[q, e] = packed[e * RP : (e + 1) * RP]

    pack(0)
    logit_buf[x, 0:8] = dot(rwt_ref[:, pl.ds(pl.multiple_of(x * 512, 512), 512)], rin_ref[...], NT)
    info = jnp.zeros((8, 128), F32)
    for row, value in enumerate(ids + pos):
        info = jnp.where(sub8 == row, jnp.where(own_lanes, value.astype(F32), 0.0), info)
    logit_buf[x, 8:16] = info

    pl.semaphore_wait(barrier, len(zpeers) + 2 * len(xpeers) + len(ypeers) + 1)

    for p in xpeers:
        send(logit_buf.at[x], logit_buf.at[x], small_s.at[0], small_r.at[0], tensor=p)

    def z_send(q):
        for d in range(HALF - 1, 0, -1):
            above, below = lax.rem(z + d, NZ), lax.rem(z + NZ - d, NZ)
            ra, rb = lax.rem(above, 3), lax.rem(below, 3)

            @pl.when(ra < 2)
            def _():
                send(
                    chunk.at[q, above // 3 * 2 + ra], zbuf.at[ra, q, d],
                    zs_sem.at[q], zr_sem.at[ra, q], expert=above,
                )

            @pl.when(rb > 0)
            def _():
                send(
                    chunk.at[q, below // 3 * 2 + rb - 1], zbuf.at[0, q, d],
                    zs_sem.at[q], zr_sem.at[0, q], expert=below,
                )

    def z_own(q):
        zbuf[0, q, 0] = chunk[q, e_lo]
        zbuf[1, q, 0] = chunk[q, e_hi]

    def z_forward(q):
        near, far = pl.ds(0, HALF), pl.ds(HALF, HALF)
        wait(zbuf.at[0, q, 1:HALF], zr_sem.at[0, q])
        cls = third // 2
        neighbour = jnp.where(third == 0, z + 1, z - 1)
        send(
            zbuf.at[0, q, near], zbuf.at[cls, q, far], fs_sem.at[0, q], fr_sem.at[cls, q], expert=neighbour
        )

        @pl.when(middle)
        def _():
            wait(zbuf.at[1, q, 1:HALF], zr_sem.at[1, q])
            send(
                zbuf.at[1, q, near], zbuf.at[0, q, far], fs_sem.at[1, q], fr_sem.at[0, q], expert=z + 1
            )

    z_own(0)
    z_send(0)
    for q in range(1, NQ):
        pack(q)
        z_own(q)

    rr, kk = iota((RH, HALF * RP), 0), iota((RH, HALF * RP), 1)
    for b in range(LB):
        relay_r[b] = onehot((kk == (rr // CAP) * RP + b * CAP + lax.rem(rr, CAP)) & (rr < HALF * CAP))
    side = jnp.where((third == 0) | ((x // 2) * sel_hi == 1), -1, 1)

    def place_of(row):
        col, in_col = row // RX, lax.rem(row, RX)
        in_half = lax.rem(in_col, RH)
        dist, slot = in_half // CAP, lax.rem(in_half, CAP)
        source = jnp.where(in_col < RH, z + side * dist, z - side - side * dist)
        return col, lax.rem(source + 2 * NZ, NZ), slot, in_half < HALF * CAP

    load(hid_hbm, hid, 0).wait()
    col, source, slot, used = place_of(iota((ROWS, NX * NZ * CAP), 0))
    perm = onehot((iota((ROWS, NX * NZ * CAP), 1) == (source * NX + col) * CAP + slot) & used)
    hidp[...] = dot(perm, hid[...]).astype(BF16)
    hidt[...] = hidp[...].T

    others = lambda ref, n: ref.at[0 : n - 1]
    wait(others(logit_buf, NX), small_r.at[0])
    shared = logit_buf[0] + logit_buf[1] + logit_buf[2] + logit_buf[3]
    logits = shared[0:8]
    ids = [shared[8 + k : 9 + k].astype(I32) for k in range(2)]
    pos = [shared[10 + k : 11 + k].astype(I32) for k in range(2)]
    hit = [sub8 == ids[k] for k in range(2)]
    picked = [jnp.sum(jnp.where(hit[k], logits, 0.0), axis=0, keepdims=True) for k in range(2)]
    gate = [jax.nn.sigmoid(picked[0] - picked[1]), jax.nn.sigmoid(picked[1] - picked[0])]
    packed_gate = dot(
        jnp.where(hit[0] & own_lanes, gate[0], 0.0).astype(BF16), onehot(r128 == pos[0]), NT
    ) + dot(jnp.where(hit[1] & own_lanes, gate[1], 0.0).astype(BF16), onehot(r128 == pos[1]), NT)
    pg_send[...] = packed_gate
    pg_buf[z] = packed_gate
    for p in zpeers:
        send(pg_send, pg_buf.at[z], small_s.at[1], small_r.at[1], expert=p)
    z_send(1)

    def z_relay(q, half):
        if half:
            wait(zbuf.at[0, q, HALF:NZ], fr_sem.at[0, q])

            @pl.when(middle)
            def _():
                wait(zbuf.at[1, q, HALF:NZ], fr_sem.at[1, q])

        for cls in range(2):
            at = 0 if cls == 0 else sel_hi
            rows = zbuf[at, q, half * HALF : (half + 1) * HALF].reshape(HALF * RP, 128)
            for b in range(LB):
                xsend[cls, q, half, :, b * 128 : (b + 1) * 128] = dot(relay_r[b], rows).astype(BF16)
        for p in xpeers:
            send(
                xsend.at[p // 2, q, half], xbuf.at[q, x, half], xs_sem.at[q], xr_sem.at[q], tensor=p
            )
        xbuf[q, x, half] = xsend[x // 2, q, half]

    z_forward(0)
    z_relay(0, 0)
    z_send(2)
    z_forward(1)

    wait(others(pg_buf, NZ), small_r.at[1])
    sub3 = iota((NZ, 8, 128), 1)
    for cls, e in ((0, e_lo), (1, e_hi)):
        pgx_send[cls] = jnp.zeros((16, 128), F32)
        pgx_send[cls, 0:NZ] = jnp.sum(jnp.where(sub3 == e, pg_buf[...], 0.0), axis=1)
    for p in xpeers:
        send(pgx_send.at[p // 2], pgx_buf.at[x], small_s.at[2], small_r.at[2], tensor=p)
    pgx_buf[x] = pgx_send[x // 2]

    z_relay(0, 1)
    z_relay(1, 0)
    z_send(3)
    z_forward(2)
    z_relay(1, 1)
    z_relay(2, 0)

    col, source, slot, used = place_of(iota((ROWS, 64), 0))
    column_of = onehot((iota((ROWS, 64), 1) == col * 16 + source) & used)
    col, source, slot, used = place_of(iota((ROWS, 128), 0))
    own_slot = iota((ROWS, 128), 1) == slot
    own_row = (iota((ROWS, 128), 1) == source * CAP + slot) & used

    def make_gates():
        wait(others(pgx_buf, NX), small_r.at[2])
        spread_gate = dot(column_of, pgx_buf[...].reshape(64, 128).astype(BF16))
        column = jnp.sum(jnp.where(own_slot, spread_gate, 0.0), axis=1, keepdims=True)
        gcol[...] = jnp.broadcast_to(column, (ROWS, 128))

    def x_wait(q):
        wait(others(xbuf.at[q], NX), xr_sem.at[q])

    def image_part(q):
        part = dot(xbuf[q].reshape(ROWS, QC), down[:, q * QC : (q + 1) * QC], NT)
        if q == 0:
            image[...] = part
        else:
            image[...] += part

    def weight_part(q):
        rows = xbuf[q].reshape(ROWS, QC).astype(F32)
        gated = (gcol[:, 0:1] * rows).astype(BF16)
        term = dot(hidt[...], gated).astype(BF16)
        for yy in range(NY):
            for cc in range(NC):
                at = (yy * NC + cc) * 80
                wbuf[q, cc, yy] = term[at : at + 80]
        send(wbuf.at[q, oc], dbuf.at[q], d_s.at[q], d_r.at[q], dp_1=oc)

    def cols(half):
        return pl.ds(half * (QC // 2), QC // 2)

    def y_send(q, src, d, half, s):
        slot = RS_SLOT[(d, half, s)]
        send(src, rsbuf.at[q, slot], rs_s.at[q], rs_r.at[q, slot], dp_0=up if d == PLUS else dn)

    def rs_first(q):
        wait(dbuf.at[q], d_r.at[q])
        dbuf[q] = (wbuf[q, c].astype(F32) + dbuf[q].astype(F32)).astype(BF16)
        for d, half, far in ((PLUS, 0, 4), (MINUS, 1, 4), (PLUS, 1, 3), (MINUS, 0, 5)):
            y_send(q, dbuf.at[q, lax.rem(y + far, NY), :, cols(half)], d, half, 0)

    def rs_step(q, s):
        for d, half, n, off in (
            (PLUS, 0, 4, 3 - s), (MINUS, 1, 4, 5 + s), (PLUS, 1, 3, 2 - s), (MINUS, 0, 3, 6 + s),
        ):
            if s >= n:
                continue
            slot = RS_SLOT[(d, half, s)]
            wait(rsbuf.at[q, slot], rs_r.at[q, slot])
            if s == n - 1:
                continue
            block = dbuf[q, lax.rem(y + off, NY), :, half * (QC // 2) : (half + 1) * (QC // 2)]
            rsbuf[q, slot] = (rsbuf[q, slot].astype(F32) + block.astype(F32)).astype(BF16)
            y_send(q, rsbuf.at[q, slot], d, half, s + 1)
        if s == 3:
            for half in range(2):
                lo = half * (QC // 2)
                a = rsbuf[q, RS_SLOT[(PLUS, half, 3 - half)]].astype(F32)
                b = rsbuf[q, RS_SLOT[(MINUS, half, 2 + half)]].astype(F32)
                mine = dbuf[q, y, :, lo : lo + QC // 2].astype(F32)
                wg_ref[:, q * QC + lo : q * QC + lo + QC // 2] = (mine + a + b).astype(BF16)

    make_gates()
    x_wait(0)
    weight_part(0)
    z_forward(3)
    z_relay(2, 1)
    z_relay(3, 0)
    load(down_hbm, down, 1).wait()
    image_part(0)
    x_wait(1)
    weight_part(1)
    z_relay(3, 1)
    rs_first(0)
    image_part(1)
    rs_first(1)
    x_wait(2)
    weight_part(2)
    rs_step(0, 0)
    image_part(2)
    x_wait(3)
    image_part(3)

    slot_sum = jnp.sum(hidp[...].astype(F32) * image[...], axis=1, keepdims=True)
    rt, lt = iota((8, ROWS), 0), iota((8, ROWS), 1)
    back = jnp.where(rt == (x // 2) * sel_hi * NX + lt // RX, 1.0, 0.0)
    gx_buf[x] = dot(back, jnp.where(own_row, slot_sum, 0.0), precision=HIGH)
    for p in xpeers:
        send(gx_buf.at[x], gx_buf.at[x], small_s.at[3], small_r.at[3], tensor=p)

    rs_step(0, 1)
    weight_part(3)
    rs_step(1, 0)
    rs_first(2)

    wait(others(gx_buf, NX), small_r.at[3])
    gz_buf[z] = gx_buf[0] + gx_buf[1] + gx_buf[2] + gx_buf[3]
    for p in zpeers:
        send(gz_buf.at[z], gz_buf.at[z], small_s.at[4], small_r.at[4], expert=p)

    rs_first(3)
    rs_step(0, 2)
    rs_step(1, 1)

    scaled = (gcol[:, 0:1] * image[...]).astype(BF16)
    col, source, slot, used = place_of(iota((NX * NZ * CAP, ROWS), 1))
    unperm = onehot((iota((NX * NZ * CAP, ROWS), 0) == (source * NX + col) * CAP + slot) & used)
    hg[...] = dot(unperm, scaled).astype(BF16)

    wait(others(gz_buf, NZ), small_r.at[4])
    sums = []
    for p in range(0, NZ, 3):
        sums.append(gz_buf[p] + gz_buf[p + 1])
        sums.append(gz_buf[p + 2] + pltpu.roll(gz_buf[p + 1], 4, 0))
    sums = jnp.concatenate(sums, axis=0)
    r64 = iota((64, 128), 0)
    gate_grad = []
    for k in range(2):
        at_slot = dot(sums, jnp.where(r128 == z * CAP + pos[k], 1.0, 0.0), precision=HIGH)
        mine = r64 == ids[k] * 8 + lane1 // TOK
        gate_grad.append(jnp.sum(jnp.where(mine, at_slot, 0.0), axis=0, keepdims=True))
    mixed = gate[0] * gate_grad[0] + gate[1] * gate_grad[1]
    logit_grad = jnp.where(hit[0], gate[0] * (gate_grad[0] - mixed), 0.0) + jnp.where(
        hit[1], gate[1] * (gate_grad[1] - mixed), 0.0
    )
    router = dot(logit_grad, rin_ref[...].astype(F32), precision=HIGH)
    rp_send[0] = router[:, 0:256]
    rp_send[1] = router[:, 256:512]
    send(rp_send.at[oc], rc_buf, small_s.at[5], small_r.at[5], dp_1=oc)

    rs_step(2, 0)
    wait(rc_buf, small_r.at[5])
    pair = rp_send[c] + rc_buf[...]
    rz_buf[z] = pair
    for p in zpeers:
        send(rz_buf.at[z], rz_buf.at[z], small_s.at[6], small_r.at[6], expert=p)

    rs_step(3, 0)
    rs_step(1, 2)
    rs_step(0, 3)
    tall[...] = jnp.concatenate([logit_grad] * 16, axis=0).T
    own_grad = tall[pl.ds(pl.multiple_of(x * TOK, TOK), TOK), 0:8]
    ig_ref[...] = dot(own_grad, rwt_ref[...].astype(F32), precision=HIGH).astype(BF16)
    rs_step(2, 1)
    rs_step(3, 1)
    rs_step(1, 3)
    wait(others(rz_buf, NZ), small_r.at[6])
    total = rz_buf[0]
    for p in range(1, NZ):
        total = total + rz_buf[p]
    ry_buf[y] = total
    for p in ypeers:
        send(ry_buf.at[y], ry_buf.at[y], small_s.at[7], small_r.at[7], dp_0=p)
    rs_step(2, 2)
    rs_step(3, 2)
    wait(others(ry_buf, NY), small_r.at[7])
    total = ry_buf[0]
    for p in range(1, NY):
        total = total + ry_buf[p]
    here = x * NC + c
    rx_buf[here] = total
    for p in xpeers:
        for cc in (c, oc):
            send(rx_buf.at[here], rx_buf.at[here], small_s.at[8], small_r.at[8], tensor=p, dp_1=cc)
    send(rx_buf.at[here], rx_buf.at[here], small_s.at[8], small_r.at[8], dp_1=oc)
    rs_step(2, 3)
    rs_step(3, 3)
    wait(others(rx_buf, NX * NC), small_r.at[8])
    for i in range(NX * NC):
        rg_ref[:, i * 256 : (i + 1) * 256] = rx_buf[i]

    for q in range(NQ):
        wait(zbuf.at[0, q, 0:HALF], fs_sem.at[0, q])

        @pl.when(middle)
        def _():
            wait(zbuf.at[0, q, 0 : NE - 2], zs_sem.at[q])
            wait(zbuf.at[1, q, 0:HALF], fs_sem.at[1, q])

        @pl.when(jnp.logical_not(middle))
        def _():
            wait(zbuf.at[0, q, 0 : NE - 1], zs_sem.at[q])

        wait(others(xbuf.at[q], NX), xs_sem.at[q])
        wait(dbuf.at[q], d_s.at[q])
        wait(rsbuf.at[q], rs_s.at[q])
    for i, (buf, n) in enumerate(
        ((logit_buf, NX), (pg_buf, NZ), (pgx_buf, NX), (gx_buf, NX), (gz_buf, NZ))
    ):
        wait(others(buf, n), small_s.at[i])
    wait(rc_buf, small_s.at[5])
    wait(others(rz_buf, NZ), small_s.at[6])
    wait(others(ry_buf, NY), small_s.at[7])
    wait(others(rx_buf, NX * NC), small_s.at[8])


def write_out(wg, hg, rg, ig, wg_out, hg_out, rg_out, ig_out, sem):
    copies = [
        pltpu.make_async_copy(src, dst, sem.at[i])
        for i, (src, dst) in enumerate(((hg, hg_out), (wg, wg_out), (ig, ig_out), (rg, rg_out)))
    ]
    for copy in copies:
        copy.start()
    for copy in copies:
        copy.wait()


def per_device(router_input, router_weight, expert_ids, down_weight, hidden, grad_output):
    ids = expert_ids.T
    rwt = router_weight.T
    slots, units = hidden.shape[1], hidden.shape[2]
    width = grad_output.shape[1]
    vmem = pl.BlockSpec(memory_space=pltpu.VMEM)
    hbm = pl.BlockSpec(memory_space=pl.ANY)
    V = pltpu.VMEM
    dma = pltpu.SemaphoreType.DMA
    results = (
        ((units // (NY * NC), width), BF16),
        ((slots, units), BF16),
        ((8, width), F32),
        ((TOK, width), BF16),
    )
    inner = pl.pallas_call(
        kernel,
        out_shape=tuple(V(shape, kind) for shape, kind in results),
        in_specs=[vmem, vmem, vmem, vmem, hbm, hbm],
        out_specs=(vmem, vmem, vmem, vmem),
        scratch_shapes=[
            V((units, width), BF16),
            V((slots, units), BF16),
            V((ROWS, units), BF16),
            V((units, ROWS), BF16),
            V((ROWS, units), F32),
            V((ROWS, 128), F32),
            V((LB, RH, HALF * RP), BF16),
            V((8, 128), I32),
            V((128, 128), F32),
            V((NQ, NE, RP, 128), BF16),
            V((2, NQ, NZ, RP, 128), BF16),
            V((2, NQ, 2, RH, QC), BF16),
            V((NQ, NX, 2, RH, QC), BF16),
            V((NX, 16, 128), F32),
            V((8, 128), F32),
            V((NZ, 8, 128), F32),
            V((2, 16, 128), F32),
            V((NX, 16, 128), F32),
            V((NX, 8, 128), F32),
            V((NZ, 8, 128), F32),
            V((2, 8, 256), F32),
            V((8, 256), F32),
            V((NY, 8, 256), F32),
            V((NZ, 8, 256), F32),
            V((NX * NC, 8, 256), F32),
            V((NQ, NC, NY, 80, QC), BF16),
            V((NQ, NY, 80, QC), BF16),
            V((NQ, NRS, 80, QC // 2), BF16),
            dma((2,)),
            dma((NQ,)), dma((2, NQ)), dma((2, NQ)), dma((2, NQ)),
            dma((NQ,)), dma((NQ,)),
            dma((9,)), dma((9,)),
            dma((NQ,)), dma((NQ,)), dma((NQ,)), dma((NQ, NRS)),
        ],
        compiler_params=pltpu.CompilerParams(
            collective_id=0, has_side_effects=True, vmem_limit_bytes=60 * 1024 * 1024
        ),
    )(ids, router_input, rwt, grad_output, down_weight, hidden[0])
    weight_grad, hidden_grad, router, input_grad = pl.pallas_call(
        write_out,
        out_shape=tuple(jax.ShapeDtypeStruct(shape, kind) for shape, kind in results),
        in_specs=[vmem] * 4,
        out_specs=(hbm,) * 4,
        scratch_shapes=[dma((4,))],
        compiler_params=pltpu.CompilerParams(vmem_limit_bytes=1024 * 1024),
    )(*inner)
    return weight_grad, hidden_grad[None], router.T, input_grad


def solution(mesh):
    finer = Mesh(
        mesh.devices.reshape(NY, NC, mesh.shape["expert"], mesh.shape["tensor"]),
        ("dp_0", "dp_1", "expert", "tensor"),
    )
    placed = (
        P(DP_EXPERT, "tensor"),
        P(),
        P(DP_EXPERT_TENSOR, None),
        P(("expert", "tensor"), None),
        P(DP, None, ("expert", "tensor")),
        P(DP_EXPERT_TENSOR, None),
    )
    return jax.shard_map(
        per_device,
        mesh=finer,
        in_specs=placed,
        out_specs=(
            P(EXPERT_TENSOR_DP, None),
            P(DP, None, ("expert", "tensor")),
            P(),
            P(DP_EXPERT_TENSOR, None),
        ),
        check_vma=False,
    )
```

```python
import functools

import jax
import jax.numpy as jnp
from jax import lax
from jax.experimental import pallas as pl
from jax.experimental.pallas import tpu as pltpu
from jax.sharding import Mesh
from jax.sharding import PartitionSpec as P

F32 = jnp.float32
BF16 = jnp.bfloat16
I32 = jnp.int32
HIGH = lax.Precision.HIGHEST
NT = (((1,), (1,)), ((), ()))

DP = ("dp_0", "dp_1")
DP_EXPERT_TENSOR = ("dp_0", "dp_1", "expert", "tensor")
DP_EXPERT = ("dp_0", "dp_1", "expert")
EXPERT_TENSOR_DP = ("expert", "tensor", "dp_0", "dp_1")

NY, NC, NZ, NX = 8, 2, 12, 4
NE = 8
CAP = 9
TOK = 32
NQ = 4
LB = 4
QC = LB * 128
RP = 40
RX = 112
ROWS = NX * RX
HALF = NZ // 2
RH = RX // 2
ZORDER = (6, 7, 5, 8, 4, 9, 3, 10, 2, 11, 1)
PLUS, MINUS = 0, 1
RS_SLOT = {}
for _s in range(4):
    for _dir, _half, _n in ((PLUS, 0, 4), (MINUS, 1, 4), (PLUS, 1, 3), (MINUS, 0, 3)):
        if _s < _n:
            RS_SLOT[(_dir, _half, _s)] = len(RS_SLOT)
NRS = len(RS_SLOT)


def iota(shape, dim):
    return lax.broadcasted_iota(I32, shape, dim)


def onehot(mask):
    return jnp.where(mask, 1.0, 0.0).astype(BF16)


def dot(a, b, dims=(((1,), (0,)), ((), ())), precision=None):
    return lax.dot_general(a, b, dims, precision=precision, preferred_element_type=F32)


def kernel(
    ids_ref, rin_ref, rwt_ref, grad_ref, down_hbm, hid_hbm,
    wg_ref, hg, rg_ref, ig_ref,
    down, hid, hidp, hidt, image, gcol, relay_r, ids_v, tall,
    chunk, zbuf, xsend, xbuf,
    logit_buf, pg_send, pg_buf, pgx_send, pgx_buf,
    gx_buf, gz_buf,
    rp_send, rc_buf, ry_buf, rz_buf, rx_buf,
    wbuf, dbuf, rsbuf,
    load_sem,
    zs_sem, zr_sem, fs_sem, fr_sem, xs_sem, xr_sem,
    small_s, small_r,
    d_s, d_r, rs_s, rs_r,
):
    y, c = lax.axis_index("dp_0"), lax.axis_index("dp_1")
    z, x = lax.axis_index("expert"), lax.axis_index("tensor")
    oc = 1 - c
    e_lo, e_hi = (z * NX) // 6, (z * NX + NX - 1) // 6
    middle = lax.rem(z, 3) == 1
    third = lax.rem(z, 3)
    sel_hi = third * (2 - third)
    zpeers = [lax.rem(z + k, NZ) for k in ZORDER]
    xpeers = [lax.rem(x + k, NX) for k in (2, 1, 3)]
    ypeers = [lax.rem(y + k, NY) for k in (4, 5, 3, 6, 2, 7, 1)]
    up, dn = lax.rem(y + 1, NY), lax.rem(y + NY - 1, NY)

    def load(src, dst, i):
        return pltpu.make_async_copy(src, dst, load_sem.at[i])

    load(hid_hbm, hid, 0).start()
    load(down_hbm, down, 1).start()

    def send(src, dst, s_sem, r_sem, **where):
        pltpu.make_async_remote_copy(
            src_ref=src, dst_ref=dst, send_sem=s_sem, recv_sem=r_sem,
            device_id=where, device_id_type=pl.DeviceIdType.MESH,
        ).start()

    def wait(ref, sem):
        pltpu.make_async_copy(ref, ref, sem).wait()

    barrier = pltpu.get_barrier_semaphore()

    def greet(**where):
        pl.semaphore_signal(barrier, inc=1, device_id=where, device_id_type=pl.DeviceIdType.MESH)

    for p in zpeers:
        greet(expert=p)
    for p in xpeers:
        greet(tensor=p)
        greet(tensor=p, dp_1=oc)
    for p in ypeers:
        greet(dp_0=p)
    greet(dp_1=oc)

    for b in range(128 // TOK):
        ids_v[0:2, b * TOK : (b + 1) * TOK] = ids_ref[...]
    sub8 = iota((8, 128), 0)
    ids = [ids_v[0:1, :], ids_v[1:2, :]]
    hit = [sub8 == ids[k] for k in range(2)]
    hits = (jnp.where(hit[0], 1.0, 0.0) + jnp.where(hit[1], 1.0, 0.0)).astype(BF16)
    r128, l128 = iota((128, 128), 0), iota((128, 128), 1)
    tri = onehot((r128 < l128) & (r128 // TOK == l128 // TOK))
    before = dot(hits, tri)
    pos = [jnp.sum(jnp.where(hit[k], before, 0.0), axis=0, keepdims=True).astype(I32) for k in range(2)]
    lane1 = iota((1, 128), 1)
    own_lanes = lane1 // TOK == x
    target = [ids[k] * RP + (lane1 // TOK) * CAP + pos[k] for k in range(2)]
    pack_rows = iota((NE * RP, 128), 0)
    table = onehot((pack_rows == target[0]) | (pack_rows == target[1]))

    def pack(q):
        stack = jnp.concatenate(
            [grad_ref[:, q * QC + b * 128 : q * QC + (b + 1) * 128] for b in range(LB)], axis=0
        )
        packed = dot(table, stack).astype(BF16)
        for e in range(NE):
            chunk[q, e] = packed[e * RP : (e + 1) * RP]

    pack(0)
    logit_buf[x, 0:8] = dot(rwt_ref[:, pl.ds(pl.multiple_of(x * 512, 512), 512)], rin_ref[...], NT)
    info = jnp.zeros((8, 128), F32)
    for row, value in enumerate(ids + pos):
        info = jnp.where(sub8 == row, jnp.where(own_lanes, value.astype(F32), 0.0), info)
    logit_buf[x, 8:16] = info

    pl.semaphore_wait(barrier, len(zpeers) + 2 * len(xpeers) + len(ypeers) + 1)

    for p in xpeers:
        send(logit_buf.at[x], logit_buf.at[x], small_s.at[0], small_r.at[0], tensor=p)

    def z_send(q):
        for d in range(HALF - 1, 0, -1):
            above, below = lax.rem(z + d, NZ), lax.rem(z + NZ - d, NZ)
            ra, rb = lax.rem(above, 3), lax.rem(below, 3)

            @pl.when(ra < 2)
            def _():
                send(
                    chunk.at[q, above // 3 * 2 + ra], zbuf.at[ra, q, d],
                    zs_sem.at[q], zr_sem.at[ra, q], expert=above,
                )

            @pl.when(rb > 0)
            def _():
                send(
                    chunk.at[q, below // 3 * 2 + rb - 1], zbuf.at[0, q, d],
                    zs_sem.at[q], zr_sem.at[0, q], expert=below,
                )

    def z_own(q):
        zbuf[0, q, 0] = chunk[q, e_lo]
        zbuf[1, q, 0] = chunk[q, e_hi]

    def z_forward(q):
        near, far = pl.ds(0, HALF), pl.ds(HALF, HALF)
        wait(zbuf.at[0, q, 1:HALF], zr_sem.at[0, q])
        cls = third // 2
        neighbour = jnp.where(third == 0, z + 1, z - 1)
        send(
            zbuf.at[0, q, near], zbuf.at[cls, q, far], fs_sem.at[0, q], fr_sem.at[cls, q], expert=neighbour
        )

        @pl.when(middle)
        def _():
            wait(zbuf.at[1, q, 1:HALF], zr_sem.at[1, q])
            send(
                zbuf.at[1, q, near], zbuf.at[0, q, far], fs_sem.at[1, q], fr_sem.at[0, q], expert=z + 1
            )

    z_own(0)
    z_send(0)
    pack(1)
    z_own(1)
    z_send(1)
    for q in range(2, NQ):
        pack(q)
        z_own(q)

    rr, kk = iota((RH, HALF * RP), 0), iota((RH, HALF * RP), 1)
    for b in range(LB):
        relay_r[b] = onehot((kk == (rr // CAP) * RP + b * CAP + lax.rem(rr, CAP)) & (rr < HALF * CAP))
    side = jnp.where((third == 0) | ((x // 2) * sel_hi == 1), -1, 1)

    def place_of(row):
        col, in_col = row // RX, lax.rem(row, RX)
        in_half = lax.rem(in_col, RH)
        dist, slot = in_half // CAP, lax.rem(in_half, CAP)
        source = jnp.where(in_col < RH, z + side * dist, z - side - side * dist)
        return col, lax.rem(source + 2 * NZ, NZ), slot, in_half < HALF * CAP

    load(hid_hbm, hid, 0).wait()
    col, source, slot, used = place_of(iota((ROWS, NX * NZ * CAP), 0))
    perm = onehot((iota((ROWS, NX * NZ * CAP), 1) == (source * NX + col) * CAP + slot) & used)
    hidp[...] = dot(perm, hid[...]).astype(BF16)
    hidt[...] = hidp[...].T

    others = lambda ref, n: ref.at[0 : n - 1]
    wait(others(logit_buf, NX), small_r.at[0])
    shared = logit_buf[0] + logit_buf[1] + logit_buf[2] + logit_buf[3]
    logits = shared[0:8]
    ids = [shared[8 + k : 9 + k].astype(I32) for k in range(2)]
    pos = [shared[10 + k : 11 + k].astype(I32) for k in range(2)]
    hit = [sub8 == ids[k] for k in range(2)]
    picked = [jnp.sum(jnp.where(hit[k], logits, 0.0), axis=0, keepdims=True) for k in range(2)]
    gate = [jax.nn.sigmoid(picked[0] - picked[1]), jax.nn.sigmoid(picked[1] - picked[0])]
    packed_gate = dot(
        jnp.where(hit[0] & own_lanes, gate[0], 0.0).astype(BF16), onehot(r128 == pos[0]), NT
    ) + dot(jnp.where(hit[1] & own_lanes, gate[1], 0.0).astype(BF16), onehot(r128 == pos[1]), NT)
    pg_send[...] = packed_gate
    pg_buf[z] = packed_gate
    for p in zpeers:
        send(pg_send, pg_buf.at[z], small_s.at[1], small_r.at[1], expert=p)
    z_send(2)

    def z_relay(q, half):
        if half:
            wait(zbuf.at[0, q, HALF:NZ], fr_sem.at[0, q])

            @pl.when(middle)
            def _():
                wait(zbuf.at[1, q, HALF:NZ], fr_sem.at[1, q])

        for cls in range(2):
            at = 0 if cls == 0 else sel_hi
            rows = zbuf[at, q, half * HALF : (half + 1) * HALF].reshape(HALF * RP, 128)
            for b in range(LB):
                xsend[cls, q, half, :, b * 128 : (b + 1) * 128] = dot(relay_r[b], rows).astype(BF16)
        for p in xpeers:
            send(
                xsend.at[p // 2, q, half], xbuf.at[q, x, half], xs_sem.at[q], xr_sem.at[q], tensor=p
            )
        xbuf[q, x, half] = xsend[x // 2, q, half]

    z_forward(0)
    z_relay(0, 0)
    z_forward(1)
    z_relay(1, 0)
    z_send(3)

    wait(others(pg_buf, NZ), small_r.at[1])
    sub3 = iota((NZ, 8, 128), 1)
    for cls, e in ((0, e_lo), (1, e_hi)):
        pgx_send[cls] = jnp.zeros((16, 128), F32)
        pgx_send[cls, 0:NZ] = jnp.sum(jnp.where(sub3 == e, pg_buf[...], 0.0), axis=1)
    for p in xpeers:
        send(pgx_send.at[p // 2], pgx_buf.at[x], small_s.at[2], small_r.at[2], tensor=p)
    pgx_buf[x] = pgx_send[x // 2]

    z_relay(0, 1)
    z_forward(2)
    z_relay(1, 1)
    z_relay(2, 0)

    col, source, slot, used = place_of(iota((ROWS, 64), 0))
    column_of = onehot((iota((ROWS, 64), 1) == col * 16 + source) & used)
    col, source, slot, used = place_of(iota((ROWS, 128), 0))
    own_slot = iota((ROWS, 128), 1) == slot
    own_row = (iota((ROWS, 128), 1) == source * CAP + slot) & used

    def make_gates():
        wait(others(pgx_buf, NX), small_r.at[2])
        spread_gate = dot(column_of, pgx_buf[...].reshape(64, 128).astype(BF16))
        column = jnp.sum(jnp.where(own_slot, spread_gate, 0.0), axis=1, keepdims=True)
        gcol[...] = jnp.broadcast_to(column, (ROWS, 128))

    def x_wait(q):
        wait(others(xbuf.at[q], NX), xr_sem.at[q])

    def image_part(q):
        part = dot(xbuf[q].reshape(ROWS, QC), down[:, q * QC : (q + 1) * QC], NT)
        if q == 0:
            image[...] = part
        else:
            image[...] += part

    def weight_part(q):
        rows = xbuf[q].reshape(ROWS, QC).astype(F32)
        gated = (gcol[:, 0:1] * rows).astype(BF16)
        term = dot(hidt[...], gated).astype(BF16)
        for yy in range(NY):
            for cc in range(NC):
                at = (yy * NC + cc) * 80
                wbuf[q, cc, yy] = term[at : at + 80]
        send(wbuf.at[q, oc], dbuf.at[q], d_s.at[q], d_r.at[q], dp_1=oc)

    def cols(half):
        return pl.ds(half * (QC // 2), QC // 2)

    def y_send(q, src, d, half, s):
        slot = RS_SLOT[(d, half, s)]
        send(src, rsbuf.at[q, slot], rs_s.at[q], rs_r.at[q, slot], dp_0=up if d == PLUS else dn)

    def rs_first(q):
        wait(dbuf.at[q], d_r.at[q])
        dbuf[q] = (wbuf[q, c].astype(F32) + dbuf[q].astype(F32)).astype(BF16)
        for d, half, far in ((PLUS, 0, 4), (MINUS, 1, 4), (PLUS, 1, 3), (MINUS, 0, 5)):
            y_send(q, dbuf.at[q, lax.rem(y + far, NY), :, cols(half)], d, half, 0)

    def rs_step(q, s):
        for d, half, n, off in (
            (PLUS, 0, 4, 3 - s), (MINUS, 1, 4, 5 + s), (PLUS, 1, 3, 2 - s), (MINUS, 0, 3, 6 + s),
        ):
            if s >= n:
                continue
            slot = RS_SLOT[(d, half, s)]
            wait(rsbuf.at[q, slot], rs_r.at[q, slot])
            if s == n - 1:
                continue
            block = dbuf[q, lax.rem(y + off, NY), :, half * (QC // 2) : (half + 1) * (QC // 2)]
            rsbuf[q, slot] = (rsbuf[q, slot].astype(F32) + block.astype(F32)).astype(BF16)
            y_send(q, rsbuf.at[q, slot], d, half, s + 1)
        if s == 3:
            for half in range(2):
                lo = half * (QC // 2)
                a = rsbuf[q, RS_SLOT[(PLUS, half, 3 - half)]].astype(F32)
                b = rsbuf[q, RS_SLOT[(MINUS, half, 2 + half)]].astype(F32)
                mine = dbuf[q, y, :, lo : lo + QC // 2].astype(F32)
                wg_ref[:, q * QC + lo : q * QC + lo + QC // 2] = (mine + a + b).astype(BF16)

    z_forward(3)
    x_wait(0)
    load(down_hbm, down, 1).wait()
    image_part(0)
    z_relay(2, 1)
    z_relay(3, 0)
    make_gates()
    weight_part(0)
    z_relay(3, 1)
    rs_first(0)
    x_wait(1)
    weight_part(1)
    image_part(1)
    rs_first(1)
    x_wait(2)
    weight_part(2)
    rs_step(0, 0)
    image_part(2)
    x_wait(3)
    image_part(3)

    slot_sum = jnp.sum(hidp[...].astype(F32) * image[...], axis=1, keepdims=True)
    rt, lt = iota((8, ROWS), 0), iota((8, ROWS), 1)
    back = jnp.where(rt == (x // 2) * sel_hi * NX + lt // RX, 1.0, 0.0)
    gx_buf[x] = dot(back, jnp.where(own_row, slot_sum, 0.0), precision=HIGH)
    for p in xpeers:
        send(gx_buf.at[x], gx_buf.at[x], small_s.at[3], small_r.at[3], tensor=p)

    rs_step(0, 1)
    weight_part(3)
    rs_step(1, 0)
    rs_first(2)

    wait(others(gx_buf, NX), small_r.at[3])
    gz_buf[z] = gx_buf[0] + gx_buf[1] + gx_buf[2] + gx_buf[3]
    for p in zpeers:
        send(gz_buf.at[z], gz_buf.at[z], small_s.at[4], small_r.at[4], expert=p)

    rs_first(3)
    rs_step(0, 2)
    rs_step(1, 1)

    scaled = (gcol[:, 0:1] * image[...]).astype(BF16)
    col, source, slot, used = place_of(iota((NX * NZ * CAP, ROWS), 1))
    unperm = onehot((iota((NX * NZ * CAP, ROWS), 0) == (source * NX + col) * CAP + slot) & used)
    hg[...] = dot(unperm, scaled).astype(BF16)

    wait(others(gz_buf, NZ), small_r.at[4])
    sums = []
    for p in range(0, NZ, 3):
        sums.append(gz_buf[p] + gz_buf[p + 1])
        sums.append(gz_buf[p + 2] + pltpu.roll(gz_buf[p + 1], 4, 0))
    sums = jnp.concatenate(sums, axis=0)
    r64 = iota((64, 128), 0)
    gate_grad = []
    for k in range(2):
        at_slot = dot(sums, jnp.where(r128 == z * CAP + pos[k], 1.0, 0.0), precision=HIGH)
        mine = r64 == ids[k] * 8 + lane1 // TOK
        gate_grad.append(jnp.sum(jnp.where(mine, at_slot, 0.0), axis=0, keepdims=True))
    mixed = gate[0] * gate_grad[0] + gate[1] * gate_grad[1]
    logit_grad = jnp.where(hit[0], gate[0] * (gate_grad[0] - mixed), 0.0) + jnp.where(
        hit[1], gate[1] * (gate_grad[1] - mixed), 0.0
    )
    router = dot(logit_grad, rin_ref[...].astype(F32), precision=HIGH)
    rp_send[0] = router[:, 0:256]
    rp_send[1] = router[:, 256:512]
    send(rp_send.at[oc], rc_buf, small_s.at[5], small_r.at[5], dp_1=oc)

    rs_step(2, 0)
    wait(rc_buf, small_r.at[5])
    pair = rp_send[c] + rc_buf[...]
    rz_buf[z] = pair
    for p in zpeers:
        send(rz_buf.at[z], rz_buf.at[z], small_s.at[6], small_r.at[6], expert=p)

    rs_step(3, 0)
    rs_step(1, 2)
    rs_step(0, 3)
    tall[...] = jnp.concatenate([logit_grad] * 16, axis=0).T
    own_grad = tall[pl.ds(pl.multiple_of(x * TOK, TOK), TOK), 0:8]
    ig_ref[...] = dot(own_grad, rwt_ref[...].astype(F32), precision=HIGH).astype(BF16)
    rs_step(2, 1)
    rs_step(3, 1)
    wait(others(rz_buf, NZ), small_r.at[6])
    total = rz_buf[0]
    for p in range(1, NZ):
        total = total + rz_buf[p]
    ry_buf[y] = total
    for p in ypeers:
        send(ry_buf.at[y], ry_buf.at[y], small_s.at[7], small_r.at[7], dp_0=p)
    rs_step(2, 2)
    rs_step(3, 2)
    wait(others(ry_buf, NY), small_r.at[7])
    total = ry_buf[0]
    for p in range(1, NY):
        total = total + ry_buf[p]
    here = x * NC + c
    rx_buf[here] = total
    for p in xpeers:
        for cc in (c, oc):
            send(rx_buf.at[here], rx_buf.at[here], small_s.at[8], small_r.at[8], tensor=p, dp_1=cc)
    send(rx_buf.at[here], rx_buf.at[here], small_s.at[8], small_r.at[8], dp_1=oc)
    rs_step(1, 3)
    rs_step(2, 3)
    rs_step(3, 3)
    wait(others(rx_buf, NX * NC), small_r.at[8])
    for i in range(NX * NC):
        rg_ref[:, i * 256 : (i + 1) * 256] = rx_buf[i]

    for q in range(NQ):
        wait(zbuf.at[0, q, 0:HALF], fs_sem.at[0, q])

        @pl.when(middle)
        def _():
            wait(zbuf.at[0, q, 0 : NE - 2], zs_sem.at[q])
            wait(zbuf.at[1, q, 0:HALF], fs_sem.at[1, q])

        @pl.when(jnp.logical_not(middle))
        def _():
            wait(zbuf.at[0, q, 0 : NE - 1], zs_sem.at[q])

        wait(others(xbuf.at[q], NX), xs_sem.at[q])
        wait(dbuf.at[q], d_s.at[q])
        wait(rsbuf.at[q], rs_s.at[q])
    for i, (buf, n) in enumerate(
        ((logit_buf, NX), (pg_buf, NZ), (pgx_buf, NX), (gx_buf, NX), (gz_buf, NZ))
    ):
        wait(others(buf, n), small_s.at[i])
    wait(rc_buf, small_s.at[5])
    wait(others(rz_buf, NZ), small_s.at[6])
    wait(others(ry_buf, NY), small_s.at[7])
    wait(others(rx_buf, NX * NC), small_s.at[8])


def write_out(wg, hg, rg, ig, wg_out, hg_out, rg_out, ig_out, sem):
    copies = [
        pltpu.make_async_copy(src, dst, sem.at[i])
        for i, (src, dst) in enumerate(((hg, hg_out), (wg, wg_out), (ig, ig_out), (rg, rg_out)))
    ]
    for copy in copies:
        copy.start()
    for copy in copies:
        copy.wait()


def per_device(router_input, router_weight, expert_ids, down_weight, hidden, grad_output):
    ids = expert_ids.T
    rwt = router_weight.T
    slots, units = hidden.shape[1], hidden.shape[2]
    width = grad_output.shape[1]
    vmem = pl.BlockSpec(memory_space=pltpu.VMEM)
    hbm = pl.BlockSpec(memory_space=pl.ANY)
    V = pltpu.VMEM
    dma = pltpu.SemaphoreType.DMA
    results = (
        ((units // (NY * NC), width), BF16),
        ((slots, units), BF16),
        ((8, width), F32),
        ((TOK, width), BF16),
    )
    inner = pl.pallas_call(
        kernel,
        out_shape=tuple(V(shape, kind) for shape, kind in results),
        in_specs=[vmem, vmem, vmem, vmem, hbm, hbm],
        out_specs=(vmem, vmem, vmem, vmem),
        scratch_shapes=[
            V((units, width), BF16),
            V((slots, units), BF16),
            V((ROWS, units), BF16),
            V((units, ROWS), BF16),
            V((ROWS, units), F32),
            V((ROWS, 128), F32),
            V((LB, RH, HALF * RP), BF16),
            V((8, 128), I32),
            V((128, 128), F32),
            V((NQ, NE, RP, 128), BF16),
            V((2, NQ, NZ, RP, 128), BF16),
            V((2, NQ, 2, RH, QC), BF16),
            V((NQ, NX, 2, RH, QC), BF16),
            V((NX, 16, 128), F32),
            V((8, 128), F32),
            V((NZ, 8, 128), F32),
            V((2, 16, 128), F32),
            V((NX, 16, 128), F32),
            V((NX, 8, 128), F32),
            V((NZ, 8, 128), F32),
            V((2, 8, 256), F32),
            V((8, 256), F32),
            V((NY, 8, 256), F32),
            V((NZ, 8, 256), F32),
            V((NX * NC, 8, 256), F32),
            V((NQ, NC, NY, 80, QC), BF16),
            V((NQ, NY, 80, QC), BF16),
            V((NQ, NRS, 80, QC // 2), BF16),
            dma((2,)),
            dma((NQ,)), dma((2, NQ)), dma((2, NQ)), dma((2, NQ)),
            dma((NQ,)), dma((NQ,)),
            dma((9,)), dma((9,)),
            dma((NQ,)), dma((NQ,)), dma((NQ,)), dma((NQ, NRS)),
        ],
        compiler_params=pltpu.CompilerParams(
            collective_id=0, has_side_effects=True, vmem_limit_bytes=60 * 1024 * 1024
        ),
    )(ids, router_input, rwt, grad_output, down_weight, hidden[0])
    weight_grad, hidden_grad, router, input_grad = pl.pallas_call(
        write_out,
        out_shape=tuple(jax.ShapeDtypeStruct(shape, kind) for shape, kind in results),
        in_specs=[vmem] * 4,
        out_specs=(hbm,) * 4,
        scratch_shapes=[dma((4,))],
        compiler_params=pltpu.CompilerParams(vmem_limit_bytes=1024 * 1024),
    )(*inner)
    return weight_grad, hidden_grad[None], router.T, input_grad


def solution(mesh):
    finer = Mesh(
        mesh.devices.reshape(NY, NC, mesh.shape["expert"], mesh.shape["tensor"]),
        ("dp_0", "dp_1", "expert", "tensor"),
    )
    placed = (
        P(DP_EXPERT, "tensor"),
        P(),
        P(DP_EXPERT_TENSOR, None),
        P(("expert", "tensor"), None),
        P(DP, None, ("expert", "tensor")),
        P(DP_EXPERT_TENSOR, None),
    )
    return jax.shard_map(
        per_device,
        mesh=finer,
        in_specs=placed,
        out_specs=(
            P(EXPERT_TENSOR_DP, None),
            P(DP, None, ("expert", "tensor")),
            P(),
            P(DP_EXPERT_TENSOR, None),
        ),
        check_vma=False,
    )
```
